32 devices in a mesh: wide: 8 (over y, x, core), tp: 4 (over z).
Axes of the slice: x: 2, y: 2, z: 4, core: 2. Of those that a mesh axis runs over, the one named last changes fastest.
Arguments:
- inputs: bfloat16 [4096, 2048], P(('wide', 'tp')), may hold values from -8 to 8
- cotangent: bfloat16 [4096, 2048], P(('wide', 'tp')), may hold values from -6 to 6
- expert_choice: int32 [4096, 6], P(('wide', 'tp')), may hold values from 0 to 15, all different within a row; in each aligned block of 128 rows (0 to 127, 128 to 255, ...) at most 56 rows name the same one
- norm1_gain: float32 [2048], replicated, may hold values from 0.5 to 1.5
- w_query: bfloat16 [2048, 3072], P(None, 'tp'), may hold values from -0.20289502 to 0.20289502
- w_latent: bfloat16 [2048, 576], replicated, may hold values from -0.20289502 to 0.20289502
- latent_gain: float32 [512], replicated, may hold values from 0.5 to 1.5
- w_keyval: bfloat16 [512, 4096], P(None, 'tp'), may hold values from -0.25 to 0.25
- w_out: bfloat16 [2048, 2048], P(None, 'tp'), may hold values from -0.5 to 0.5
- norm2_gain: float32 [2048], replicated, may hold values from 0.5 to 1.5
- w_router: bfloat16 [2048, 16], replicated, may hold values from -0.125 to 0.125
- w_shared_gate: bfloat16 [2048, 2816], P(None, 'tp'), may hold values from -0.125 to 0.125
- w_shared_up: bfloat16 [2048, 2816], P(None, 'tp'), may hold values from -0.125 to 0.125
- w_shared_down: bfloat16 [2048, 2816], P(None, 'tp'), may hold values from -0.109375 to 0.109375
- w_expert_gate: bfloat16 [16, 2048, 1408], P('wide', None, 'tp'), may hold values from -0.125 to 0.125
- w_expert_up: bfloat16 [16, 2048, 1408], P('wide', None, 'tp'), may hold values from -0.125 to 0.125
- w_expert_down: bfloat16 [16, 2048, 1408], P('wide', None, 'tp'), may hold values from -0.15625 to 0.15625
Outputs:
- output: float32 [4096, 2048], P(('wide', 'tp'))
- grad_input: float32 [4096, 2048], P(('wide', 'tp'))
- grad_norm1_gain: float32 [2048], P(('wide', 'tp'))
- grad_query: float32 [2048, 3072], P('wide', 'tp')
- grad_latent: float32 [2048, 576], P(('wide', 'tp'))
- grad_latent_gain: float32 [512], P(('wide', 'tp'))
- grad_keyval: float32 [512, 4096], P('wide', 'tp')
- grad_out: float32 [2048, 2048], P('wide', 'tp')
- grad_norm2_gain: float32 [2048], P(('wide', 'tp'))
- grad_router: float32 [2048, 16], P(('wide', 'tp'))
- grad_shared_gate: float32 [2048, 2816], P('wide', 'tp')
- grad_shared_up: float32 [2048, 2816], P('wide', 'tp')
- grad_shared_down: float32 [2048, 2816], P('wide', 'tp')
- grad_expert_gate: float32 [16, 2048, 1408], P('wide', None, 'tp')
- grad_expert_up: float32 [16, 2048, 1408], P('wide', None, 'tp')
- grad_expert_down: float32 [16, 2048, 1408], P('wide', None, 'tp')
The draws below stay inside these ranges and needn't reach their ends.
Inputs may be any that keep to these rules, and one draw needn't show every extreme that they name: `expert_choice`: each row names 6 different experts. Within each device's block of 128 rows no expert is named by more than 56 rows, and in some blocks one expert is named by exactly 56 rows.
All inputs are finite; a program needn't handle non-finite values.
Results may differ from the reference program's by a relative error of at most 0.033.
Values may be sent and summed in bfloat16 or wider, within the bound.
A program may use at most 576 MiB of HBM per device.

```python
import math
import jax
import jax.numpy as jnp
import numpy as np
from jax import lax

D = 2048
HEADS = 16
NOPE = 128
ROPE = 64
VDIM = 128
RANK = 512
EFF = 1408
SFF = 2816
TOP = 6
SEQ = 512
EXPERTS = 16
TOK_DEV = 128
TOKENS = 4096
CAP = 56
N_WIDE = 8


def weight_values_keyed(key, salt, column_total):
    weight_scale = D ** (-0.5)
    bound_value = 6.0 * D ** (-0.5) + 144.0 * D ** (-1.0)
    own_key = jax.random.fold_in(key, salt)
    values = jnp.clip(jax.random.normal(own_key, (D, column_total), jnp.float32), -6.0, 6.0) * weight_scale
    return jnp.clip(values, -bound_value, bound_value)


def draw_w_query(key, part):
    return weight_values_keyed(key, 31, HEADS * (NOPE + ROPE)).astype(jnp.bfloat16)


def draw_w_latent(key, part):
    return weight_values_keyed(key, 41, RANK + ROPE).astype(jnp.bfloat16)


def draw_inputs(key, part):
    values = jax.random.normal(jax.random.fold_in(key, 11), (TOKENS, D), jnp.float32)
    return jnp.clip(values, -8.0, 8.0).astype(jnp.bfloat16)


def block_levels(key, extent, pieces, least, high):
    def one(axis_at, shards_of):
        steps = jax.random.uniform(jax.random.fold_in(jax.random.fold_in(key, 6), axis_at), (shards_of,), jnp.float32, least / len(pieces), high / len(pieces))
        return jnp.repeat(jnp.exp(steps), extent[axis_at] // shards_of).reshape((-1,) + (1,) * (len(extent) - axis_at - 1))

    gain = one(*pieces[0])
    for cut in pieces[1:]:
        gain = gain * one(*cut)
    return gain


def shared_out(rng, own, number, rows, count, top, bound, lean):
    sequence = jax.random.permutation(rng, count)
    crowded, common = portions_of(count, rows * top, bound, lean, True), portions_of(count, rows * top, bound, lean, False)
    places = jnp.arange(count)

    def named(lengths, offset_by):
        used = int((lengths > 0).sum())
        fixed = max(1, used // 4)
        moved = fixed + (places - fixed + offset_by * (used - fixed)) % max(1, count - fixed)
        return jnp.zeros((count,), jnp.int32).at[sequence[jnp.where(places < fixed, places, moved)]].set(jnp.asarray(lengths, jnp.int32))

    lengths = jnp.where(number % 4 == 0, named(crowded, number // 4), named(common, number - number // 4 - 1))
    mixed = jax.random.permutation(jax.random.fold_in(own, 3), count)
    donor, receiver = mixed[0:count // 2 * 2:2], mixed[1:count // 2 * 2:2]
    room = jnp.minimum(lengths[donor] - 1, bound - lengths[receiver]) // 2
    room = jnp.where((donor == sequence[0]) | (receiver == sequence[0]) | (lengths[receiver] == 0), 0, jnp.maximum(room, 0))
    moved = jax.random.randint(jax.random.fold_in(own, 4), (count // 2,), 0, 1 << 20) % (room + 1)
    lengths = lengths.at[donor].add(-moved).at[receiver].add(moved)
    labels = jnp.searchsorted(jnp.cumsum(lengths), jnp.arange(rows * top), side="right").astype(jnp.int32)
    table = labels.reshape(top, rows).T
    table = table[jax.random.permutation(jax.random.fold_in(own, 1), rows)]
    offset_by = jax.random.randint(jax.random.fold_in(own, 2), (rows, 1), 0, top)
    return jnp.take_along_axis(table, (jnp.arange(top)[None, :] + offset_by) % top, axis=1)


def portions_of(count, total, most, slope, full):
    portions = [(1 << 20) // math.isqrt(standing ** slope) + 1 for standing in range(1, count + 1)]
    largest = most if full else min(most, max(-(-total // count), total * portions[0] // sum(portions)))
    least = 1 if total - largest >= count - 1 else 0
    given, rest = [largest] + [least] * (count - 1), total - largest - least * (count - 1)
    while rest > 0:
        movable = [i for i in range(1, count) if given[i] < largest] or [i for i in range(1, count) if given[i] < most]
        pool, budget = sum([portions[i] for i in movable]), rest
        for i in movable:
            extra = min(most - given[i], max(1, budget * portions[i] // pool), rest)
            given[i] = given[i] + extra
            rest = rest - extra
    return np.array(given)


def bell_draw(stream_key, extent, spread, reach, split=(), held_as=jnp.bfloat16):
    gain = block_levels(stream_key, extent, split, -0.22, 0.18) if split else 1.0
    values = jax.random.normal(stream_key, extent, jnp.float32) * spread * gain
    return jnp.minimum(jnp.maximum(values, -reach), reach).astype(held_as)


def setup_inputs(seed: int = 0) -> dict:
    streams_of = jax.random.split(jax.random.key(seed), 18)
    inputs = draw_inputs(jax.random.fold_in(streams_of[17], 71), 0)
    cotangent = bell_draw(streams_of[1], (TOKENS, D), 1.0, 6.0, ((0, 32),))
    expert_choice_keys = jax.random.split(jax.random.fold_in(streams_of[2], 1), TOKENS // TOK_DEV)
    expert_choice_turns = jax.random.permutation(jax.random.fold_in(streams_of[2], 3), TOKENS // TOK_DEV)
    expert_choice = jax.vmap(lambda own, number: shared_out(jax.random.fold_in(streams_of[2], 2), own, number, TOK_DEV, EXPERTS, TOP, CAP, 1))(expert_choice_keys, expert_choice_turns).reshape((TOKENS, TOP))
    norm1_gain = jnp.clip(1.0 + 0.1 * jax.random.normal(streams_of[3], (D,), jnp.float32), 0.5, 1.5)
    w_query = draw_w_query(jax.random.fold_in(streams_of[17], 71), 0)
    w_latent = draw_w_latent(jax.random.fold_in(streams_of[17], 71), 0)
    latent_gain = jnp.clip(1.0 + 0.1 * jax.random.normal(streams_of[6], (RANK,), jnp.float32), 0.5, 1.5)
    w_keyval = bell_draw(streams_of[7], (RANK, HEADS * (NOPE + VDIM)), RANK ** -0.5, 0.25, ((1, 4),))
    w_out = bell_draw(streams_of[8], (D, HEADS * VDIM), VDIM ** -0.5, 0.5, ((1, 4),))
    norm2_gain = jnp.clip(1.0 + 0.1 * jax.random.normal(streams_of[9], (D,), jnp.float32), 0.5, 1.5)
    w_router = bell_draw(streams_of[10], (D, EXPERTS), D ** -0.5, 0.125)
    w_shared_gate = bell_draw(streams_of[11], (D, SFF), D ** -0.5, 0.125, ((1, 4),))
    w_shared_up = bell_draw(streams_of[12], (D, SFF), D ** -0.5, 0.125, ((1, 4),))
    w_shared_down = bell_draw(streams_of[13], (D, SFF), SFF ** -0.5, 0.109375, ((1, 4),))
    w_expert_gate = bell_draw(streams_of[14], (EXPERTS, D, EFF), D ** -0.5, 0.125, ((0, 8), (2, 4)))
    w_expert_up = bell_draw(streams_of[15], (EXPERTS, D, EFF), D ** -0.5, 0.125, ((0, 8), (2, 4)))
    w_expert_down = bell_draw(streams_of[16], (EXPERTS, D, EFF), EFF ** -0.5, 0.15625, ((0, 8), (2, 4)))
    return dict(inputs=inputs, cotangent=cotangent, expert_choice=expert_choice, norm1_gain=norm1_gain, w_query=w_query, w_latent=w_latent, latent_gain=latent_gain, w_keyval=w_keyval, w_out=w_out, norm2_gain=norm2_gain, w_router=w_router, w_shared_gate=w_shared_gate, w_shared_up=w_shared_up, w_shared_down=w_shared_down, w_expert_gate=w_expert_gate, w_expert_up=w_expert_up, w_expert_down=w_expert_down)


EPSILON = 1e-06
ROUTE_SCALE = 2.446
THETA = 50000.0
HIGHEST = lax.Precision.HIGHEST

def product(form, left, right):
    return jnp.einsum(form, left.astype(jnp.float32), right.astype(jnp.float32))

def matmul_t(left, right):
    return lax.dot_general(left, right, (((1,), (1,)), ((), ())), preferred_element_type=jnp.float32)

def matmul_rows(left, right):
    return lax.dot_general(left, right, (((0,), (0,)), ((), ())), preferred_element_type=jnp.float32)

def rotary_tables(positions):
    half_width = ROPE // 2
    position = jnp.arange(positions, dtype=jnp.float32)[:, None]
    inverse = THETA ** (-jnp.arange(half_width, dtype=jnp.float32) / half_width)
    angle = position * inverse[None, :]
    return (jnp.cos(angle), jnp.sin(angle))

def rotate(vector, cosine, sine, turn):
    half_width = vector.shape[-1] // 2
    lower = vector[..., :half_width]
    upper = vector[..., half_width:]
    return jnp.concatenate([lower * cosine - turn * upper * sine, upper * cosine + turn * lower * sine], axis=-1)

def rms_forward(vector, gain_vector):
    inv_scale = lax.rsqrt(lax.optimization_barrier(jnp.mean(vector * vector, axis=-1, keepdims=True)) + EPSILON)
    unit_rows = vector * inv_scale
    return (unit_rows, inv_scale, unit_rows * gain_vector)

def rms_backward(grad_normed, unit_rows, inv_scale, gain_vector):
    scaled = grad_normed * gain_vector
    grad_in = inv_scale * (scaled - unit_rows * lax.optimization_barrier(jnp.mean(scaled * unit_rows, axis=-1, keepdims=True)))
    return (grad_in, lax.optimization_barrier(jnp.sum(grad_normed * unit_rows, axis=0)))

def score_block(row_total):
    return 512 if row_total % 512 == 0 else row_total

def masked_scores(query_block, key_nope, key_rope, block_start):
    query_total = query_block.shape[0]
    key_total = key_nope.shape[0]
    scores = product('qhd,khd->hqk', query_block[..., :NOPE], key_nope)
    scores = scores + product('qhd,kd->hqk', query_block[..., NOPE:], key_rope)
    scores = scores * (NOPE + ROPE) ** (-0.5)
    query_pos = block_start + jnp.arange(query_total, dtype=jnp.int32)[:, None]
    key_pos = jnp.arange(key_total, dtype=jnp.int32)[None, :]
    return jnp.where((key_pos <= query_pos)[None], scores, -1e+30)

def attention_forward(normed_b, w_query, w_latent, latent_gain, w_keyval, cosine, sine):
    row_total = normed_b.shape[0]
    head_count = w_keyval.shape[1] // (NOPE + VDIM)
    query_full = jnp.dot(normed_b, w_query, preferred_element_type=jnp.float32).reshape(row_total, head_count, NOPE + ROPE)
    query_b = jnp.concatenate([query_full[..., :NOPE], rotate(query_full[..., NOPE:], cosine[:, None, :], sine[:, None, :], 1.0)], axis=-1).astype(jnp.bfloat16)
    latent = jnp.dot(normed_b, w_latent, preferred_element_type=jnp.float32)
    key_rope = rotate(latent[:, RANK:], cosine, sine, 1.0).astype(jnp.bfloat16)
    latent_unit, latent_scale, latent_normed = rms_forward(latent[:, :RANK], latent_gain)
    latent_b = latent_normed.astype(jnp.bfloat16)
    keyval = jnp.dot(latent_b, w_keyval, preferred_element_type=jnp.float32).reshape(row_total, head_count, NOPE + VDIM).astype(jnp.bfloat16)
    key_nope = keyval[..., :NOPE]
    value_rows = keyval[..., NOPE:]
    block_rows = score_block(row_total)
    outputs = []
    sums = []
    for block_index in range(row_total // block_rows):
        block_start = block_index * block_rows
        scores = masked_scores(query_b[block_start:block_start + block_rows], key_nope, key_rope, block_start)
        row_max = lax.optimization_barrier(jnp.max(scores, axis=-1, keepdims=True))
        log_total = row_max + jnp.log(lax.optimization_barrier(jnp.sum(jnp.exp(scores - row_max), axis=-1, keepdims=True)))
        prob_b = jnp.exp(scores - log_total).astype(jnp.bfloat16)
        outputs.append(product('hqk,khd->qhd', prob_b, value_rows).astype(jnp.bfloat16))
        sums.append(log_total)
    attn_b = jnp.concatenate(outputs, axis=0).reshape(row_total, head_count * VDIM)
    log_sums = jnp.concatenate(sums, axis=1)
    return (query_b, key_rope, latent_unit, latent_scale, latent_b, key_nope, value_rows, attn_b, log_sums)

def attention_backward(grad_attn_b, normed_b, saved, w_query, w_latent, latent_gain, w_keyval, cosine, sine):
    query_b, key_rope, latent_unit, latent_scale, latent_b, key_nope, value_rows, attn_b, log_sums = saved
    row_total = normed_b.shape[0]
    head_count = key_nope.shape[1]
    grad_rows = grad_attn_b.reshape(row_total, head_count, VDIM)
    attn_rows = attn_b.reshape(row_total, head_count, VDIM)
    grad_value = jnp.zeros((row_total, head_count, VDIM), jnp.float32)
    grad_key_nope = jnp.zeros((row_total, head_count, NOPE), jnp.float32)
    grad_key_rope = jnp.zeros((row_total, ROPE), jnp.float32)
    grad_queries = []
    block_rows = score_block(row_total)
    for block_index in range(row_total // block_rows):
        block_start = block_index * block_rows
        block_end = block_start + block_rows
        query_block = query_b[block_start:block_end]
        scores = masked_scores(query_block, key_nope, key_rope, block_start)
        probs = jnp.exp(scores - log_sums[:, block_start:block_end])
        prob_b = probs.astype(jnp.bfloat16)
        grad_block = grad_rows[block_start:block_end]
        grad_value = grad_value + product('hqk,qhd->khd', prob_b, grad_block)
        grad_probs = product('qhd,khd->hqk', grad_block, value_rows)
        row_delta = lax.optimization_barrier(jnp.sum(grad_block.astype(jnp.float32) * attn_rows[block_start:block_end].astype(jnp.float32), axis=-1))
        grad_scores = (probs * (grad_probs - jnp.transpose(row_delta)[..., None]) * (NOPE + ROPE) ** (-0.5)).astype(jnp.bfloat16)
        grad_query_nope = product('hqk,khd->qhd', grad_scores, key_nope)
        grad_query_rope = product('hqk,kd->qhd', grad_scores, key_rope)
        grad_queries.append(jnp.concatenate([grad_query_nope, rotate(grad_query_rope, cosine[block_start:block_end, None, :], sine[block_start:block_end, None, :], -1.0)], axis=-1))
        grad_key_nope = grad_key_nope + product('hqk,qhd->khd', grad_scores, query_block[..., :NOPE])
        grad_key_rope = grad_key_rope + product('hqk,qhd->kd', grad_scores, query_block[..., NOPE:])
    grad_query_b = jnp.concatenate(grad_queries, axis=0).reshape(row_total, head_count * (NOPE + ROPE)).astype(jnp.bfloat16)
    grad_keyval_b = jnp.concatenate([grad_key_nope, grad_value], axis=-1).reshape(row_total, head_count * (NOPE + VDIM)).astype(jnp.bfloat16)
    grad_query_w = matmul_rows(normed_b, grad_query_b)
    grad_keyval_w = matmul_rows(latent_b, grad_keyval_b)
    grad_latent_normed = matmul_t(grad_keyval_b, w_keyval)
    grad_latent_core, grad_latent_gain = rms_backward(grad_latent_normed, latent_unit, latent_scale, latent_gain)
    grad_latent_rows = jnp.concatenate([grad_latent_core, rotate(grad_key_rope, cosine, sine, -1.0)], axis=-1)
    normed_f = normed_b.astype(jnp.float32)
    grad_latent_w = jnp.dot(normed_f.T, grad_latent_rows, precision=HIGHEST)
    grad_normed = matmul_t(grad_query_b, w_query) + jnp.dot(grad_latent_rows, w_latent.astype(jnp.float32).T, precision=HIGHEST)
    return (grad_normed, grad_query_w, grad_latent_w, grad_latent_gain, grad_keyval_w)

def gate_values(logits, onehot):
    chosen = lax.optimization_barrier(jnp.sum(onehot * logits[:, None, :], axis=-1))
    selected = jax.nn.sigmoid(chosen)
    sel_total = lax.optimization_barrier(jnp.sum(selected, axis=1, keepdims=True))
    return (ROUTE_SCALE * selected / sel_total, selected, sel_total)

def router_backward(grad_gate, selected, sel_total, onehot):
    weighted = lax.optimization_barrier(jnp.sum(grad_gate * selected, axis=1, keepdims=True))
    grad_selected = ROUTE_SCALE * (grad_gate / sel_total - weighted / (sel_total * sel_total))
    grad_chosen = grad_selected * selected * (1.0 - selected)
    return lax.optimization_barrier(jnp.sum(grad_chosen[..., None] * onehot, axis=1))

def slot_table(routes, block_rows, expert_total, capacity):
    row_total = routes.shape[0]
    top_count = routes.shape[1]
    block_total = row_total // block_rows
    grouped = routes.reshape(block_total, block_rows * top_count)
    onehot = (grouped[..., None] == jnp.arange(expert_total, dtype=jnp.int32)).astype(jnp.int32)
    earlier = jnp.cumsum(onehot, axis=1) - onehot
    slot_index = lax.optimization_barrier(jnp.sum(earlier * onehot, axis=-1))
    block_base = jnp.arange(block_total, dtype=jnp.int32)[:, None] * capacity
    flat_index = grouped * (block_total * capacity) + block_base + slot_index
    return (flat_index.reshape(row_total, top_count), slot_index.reshape(row_total, top_count))

def shared_forward(normed_b, gate_w, up_w):
    pre_gate = jnp.dot(normed_b, gate_w, preferred_element_type=jnp.float32)
    pre_up = jnp.dot(normed_b, up_w, preferred_element_type=jnp.float32)
    sigma_gate = jax.nn.sigmoid(pre_gate)
    activated = pre_gate * sigma_gate
    return (pre_gate, pre_up, sigma_gate, activated, (activated * pre_up).astype(jnp.bfloat16))

def reference(inputs, cotangent, expert_choice, norm1_gain, w_query, w_latent, latent_gain, w_keyval, w_out, norm2_gain, w_router, w_shared_gate, w_shared_up, w_shared_down, w_expert_gate, w_expert_up, w_expert_down):
    cosine, sine = rotary_tables(SEQ)
    block_total = TOKENS // TOK_DEV
    slot_rows = block_total * CAP
    flat_index, slot_index = slot_table(expert_choice, TOK_DEV, EXPERTS, CAP)
    seq_inputs = inputs.reshape(N_WIDE, SEQ, D)

    def mixer(input_rows):
        input_f = input_rows.astype(jnp.float32)
        unit1, scale1, normed1 = rms_forward(input_f, norm1_gain)
        normed1_b = normed1.astype(jnp.bfloat16)
        saved = attention_forward(normed1_b, w_query, w_latent, latent_gain, w_keyval, cosine, sine)
        hidden = input_f + matmul_t(saved[7], w_out)
        unit2, scale2, normed2 = rms_forward(hidden, norm2_gain)
        return (unit1, scale1, normed1_b, saved, hidden, unit2, scale2, normed2.astype(jnp.bfloat16))
    normed2_all = lax.map(lambda input_rows: mixer(input_rows)[7], seq_inputs).reshape(TOKENS, D)
    onehot_all = (expert_choice[..., None] == jnp.arange(EXPERTS, dtype=jnp.int32)).astype(jnp.float32)
    logits_all = jnp.dot(normed2_all, w_router, preferred_element_type=jnp.float32)
    gate_all = gate_values(logits_all, onehot_all)[0]
    grad_rows_b = (gate_all[..., None] * cotangent.astype(jnp.float32)[:, None, :]).astype(jnp.bfloat16)
    flat_rows = flat_index.reshape(-1)
    send_rows = jnp.zeros((EXPERTS * slot_rows, D), jnp.bfloat16).at[flat_rows].set(jnp.repeat(normed2_all, TOP, axis=0)).reshape(EXPERTS, slot_rows, D)
    grad_send = jnp.zeros((EXPERTS * slot_rows, D), jnp.bfloat16).at[flat_rows].set(grad_rows_b.reshape(-1, D)).reshape(EXPERTS, slot_rows, D)

    def expert_pass(expert_item):
        rows_in, rows_grad, gate_w, up_w, down_w = expert_item
        pre_gate = jnp.dot(rows_in, gate_w, preferred_element_type=jnp.float32)
        pre_up = jnp.dot(rows_in, up_w, preferred_element_type=jnp.float32)
        sigma_gate = jax.nn.sigmoid(pre_gate)
        activated = pre_gate * sigma_gate
        hidden_b = (activated * pre_up).astype(jnp.bfloat16)
        result = matmul_t(hidden_b, down_w)
        grad_hidden = jnp.dot(rows_grad, down_w, preferred_element_type=jnp.float32)
        grad_gate_b = (grad_hidden * pre_up * sigma_gate * (1.0 + pre_gate * (1.0 - sigma_gate))).astype(jnp.bfloat16)
        grad_up_b = (grad_hidden * activated).astype(jnp.bfloat16)
        grad_down_w = matmul_rows(rows_grad, hidden_b)
        grad_gate_w = matmul_rows(rows_in, grad_gate_b)
        grad_up_w = matmul_rows(rows_in, grad_up_b)
        grad_in = matmul_t(grad_gate_b, gate_w) + matmul_t(grad_up_b, up_w)
        return (result, grad_in, grad_gate_w, grad_up_w, grad_down_w)
    expert_out, expert_grad, grad_expert_gate, grad_expert_up, grad_expert_down = lax.map(expert_pass, (send_rows, grad_send, w_expert_gate, w_expert_up, w_expert_down))
    expert_out = expert_out.reshape(EXPERTS * slot_rows, D)
    expert_grad = expert_grad.reshape(EXPERTS * slot_rows, D)

    def second_pass(totals, seq_item):
        input_rows, cot_rows, flat_seq, route_seq = seq_item
        unit1, scale1, normed1_b, saved, hidden, unit2, scale2, normed2_b = mixer(input_rows)
        onehot = (route_seq[..., None] == jnp.arange(EXPERTS, dtype=jnp.int32)).astype(jnp.float32)
        logits = jnp.dot(normed2_b, w_router, preferred_element_type=jnp.float32)
        gate_weights, selected, sel_total = gate_values(logits, onehot)
        expert_rows = expert_out[flat_seq.reshape(-1)].reshape(SEQ, TOP, D)
        pre_gate, pre_up, sigma_gate, activated, shared_b = shared_forward(normed2_b, w_shared_gate, w_shared_up)
        output = hidden + matmul_t(shared_b, w_shared_down) + lax.optimization_barrier(jnp.sum(gate_weights[..., None] * expert_rows, axis=1))
        cot_f = cot_rows.astype(jnp.float32)
        grad_gate = lax.optimization_barrier(jnp.sum(expert_rows * cot_f[:, None, :], axis=-1))
        grad_routed = lax.optimization_barrier(jnp.sum(expert_grad[flat_seq.reshape(-1)].reshape(SEQ, TOP, D), axis=1))
        grad_logits = router_backward(grad_gate, selected, sel_total, onehot)
        grad_router = jnp.dot(normed2_b.astype(jnp.float32).T, grad_logits, precision=HIGHEST)
        grad_shared_hidden = jnp.dot(cot_rows, w_shared_down, preferred_element_type=jnp.float32)
        grad_pre_gate_b = (grad_shared_hidden * pre_up * sigma_gate * (1.0 + pre_gate * (1.0 - sigma_gate))).astype(jnp.bfloat16)
        grad_pre_up_b = (grad_shared_hidden * activated).astype(jnp.bfloat16)
        grad_sd = matmul_rows(cot_rows, shared_b)
        grad_sg = matmul_rows(normed2_b, grad_pre_gate_b)
        grad_su = matmul_rows(normed2_b, grad_pre_up_b)
        grad_normed2 = grad_routed + jnp.dot(grad_logits, w_router.astype(jnp.float32).T, precision=HIGHEST)
        grad_normed2 = grad_normed2 + matmul_t(grad_pre_gate_b, w_shared_gate) + matmul_t(grad_pre_up_b, w_shared_up)
        grad_h2, grad_g2 = rms_backward(grad_normed2, unit2, scale2, norm2_gain)
        grad_hidden = cot_f + grad_h2
        grad_hidden_b = grad_hidden.astype(jnp.bfloat16)
        grad_wo = matmul_rows(grad_hidden_b, saved[7])
        grad_attn_b = jnp.dot(grad_hidden_b, w_out, preferred_element_type=jnp.float32).astype(jnp.bfloat16)
        grad_normed1, grad_wq, grad_wlat, grad_lgain, grad_wkv = attention_backward(grad_attn_b, normed1_b, saved, w_query, w_latent, latent_gain, w_keyval, cosine, sine)
        grad_x1, grad_g1 = rms_backward(grad_normed1, unit1, scale1, norm1_gain)
        grad_input = grad_hidden + grad_x1
        terms = (grad_g1, grad_wq, grad_wlat, grad_lgain, grad_wkv, grad_wo, grad_g2, grad_router, grad_sg, grad_su, grad_sd)
        totals = tuple((total_item + term for total_item, term in zip(totals, terms)))
        return (totals, (output, grad_input))
    initial = (jnp.zeros((D,), jnp.float32), jnp.zeros(w_query.shape, jnp.float32), jnp.zeros(w_latent.shape, jnp.float32), jnp.zeros((RANK,), jnp.float32), jnp.zeros(w_keyval.shape, jnp.float32), jnp.zeros(w_out.shape, jnp.float32), jnp.zeros((D,), jnp.float32), jnp.zeros(w_router.shape, jnp.float32), jnp.zeros(w_shared_gate.shape, jnp.float32), jnp.zeros(w_shared_up.shape, jnp.float32), jnp.zeros(w_shared_down.shape, jnp.float32))
    seq_items = (seq_inputs, cotangent.reshape(N_WIDE, SEQ, D), flat_index.reshape(N_WIDE, SEQ, TOP), expert_choice.reshape(N_WIDE, SEQ, TOP))
    totals, stacked = lax.scan(second_pass, initial, seq_items)
    output = stacked[0].reshape(TOKENS, D)
    grad_input = stacked[1].reshape(TOKENS, D)
    return (output, grad_input, totals[0], totals[1], totals[2], totals[3], totals[4], totals[5], totals[6], totals[7], totals[8], totals[9], totals[10], grad_expert_gate, grad_expert_up, grad_expert_down)
```

```python
import jax
import jax.numpy as jnp
from jax import lax
from jax.experimental import pallas as pl
from jax.experimental.pallas import tpu as pltpu
from jax.sharding import PartitionSpec as P

NOPE = 128
ROPE = 64
VDIM = 128
RANK = 512


EPSILON = 1e-06
ROUTE_SCALE = 2.446
THETA = 50000.0
HIGHEST = lax.Precision.HIGHEST


def product(form, left, right):
    return jnp.einsum(form, left, right, preferred_element_type=jnp.float32)


def matmul_t(left, right):
    return lax.dot_general(
        left, right, (((1,), (1,)), ((), ())), preferred_element_type=jnp.float32
    )


def matmul_rows(left, right):
    return lax.dot_general(
        left, right, (((0,), (0,)), ((), ())), preferred_element_type=jnp.float32
    )


def rotary_tables(positions):
    half_width = ROPE // 2
    position = jnp.arange(positions, dtype=jnp.float32)[:, None]
    inverse = THETA ** (-jnp.arange(half_width, dtype=jnp.float32) / half_width)
    angle = position * inverse[None, :]
    return (jnp.cos(angle), jnp.sin(angle))


def rotate(vector, cosine, sine, turn):
    half_width = vector.shape[-1] // 2
    lower = vector[..., :half_width]
    upper = vector[..., half_width:]
    return jnp.concatenate(
        [lower * cosine - turn * upper * sine, upper * cosine + turn * lower * sine], axis=-1
    )


def rms_forward(vector, gain_vector):
    inv_scale = lax.rsqrt(jnp.mean(vector * vector, axis=-1, keepdims=True) + EPSILON)
    unit_rows = vector * inv_scale
    return (unit_rows, inv_scale, unit_rows * gain_vector)


def rms_backward(grad_normed, unit_rows, inv_scale, gain_vector):
    scaled = grad_normed * gain_vector
    grad_in = inv_scale * (
        scaled - unit_rows * jnp.mean(scaled * unit_rows, axis=-1, keepdims=True)
    )
    return (grad_in, jnp.sum(grad_normed * unit_rows, axis=0))


def score_block():
    return 512


def masked_scores(query_block, key_nope, key_rope):
    query_total = query_block.shape[0]
    key_total = key_nope.shape[0]
    scores = product("qhd,khd->hqk", query_block[..., :NOPE], key_nope)
    scores = scores + product("qhd,kd->hqk", query_block[..., NOPE:], key_rope)
    scores = scores * (NOPE + ROPE) ** (-0.5)
    query_pos = jnp.arange(query_total, dtype=jnp.int32)[:, None]
    key_pos = jnp.arange(key_total, dtype=jnp.int32)[None, :]
    return jnp.where((key_pos <= query_pos)[None], scores, -1e30)


def attention_forward(normed_b, w_query, w_latent, latent_gain, w_keyval, cosine, sine):
    row_total = normed_b.shape[0]
    head_count = w_keyval.shape[1] // (NOPE + VDIM)
    query_full = jnp.dot(normed_b, w_query, preferred_element_type=jnp.float32).reshape(
        row_total, head_count, NOPE + ROPE
    )
    query_b = jnp.concatenate(
        [
            query_full[..., :NOPE],
            rotate(query_full[..., NOPE:], cosine[:, None, :], sine[:, None, :], 1.0),
        ],
        axis=-1,
    ).astype(jnp.bfloat16)
    latent = jnp.dot(normed_b, w_latent, preferred_element_type=jnp.float32)
    key_rope = rotate(latent[:, RANK:], cosine, sine, 1.0).astype(jnp.bfloat16)
    latent_unit, latent_scale, latent_normed = rms_forward(latent[:, :RANK], latent_gain)
    latent_b = latent_normed.astype(jnp.bfloat16)
    keyval = (
        jnp.dot(latent_b, w_keyval, preferred_element_type=jnp.float32)
        .reshape(row_total, head_count, NOPE + VDIM)
        .astype(jnp.bfloat16)
    )
    key_nope = keyval[..., :NOPE]
    value_rows = keyval[..., NOPE:]
    scores = masked_scores(query_b, key_nope, key_rope)
    row_max = jnp.max(scores, axis=-1, keepdims=True)
    log_total = row_max + jnp.log(jnp.sum(jnp.exp(scores - row_max), axis=-1, keepdims=True))
    prob_b = jnp.exp(scores - log_total).astype(jnp.bfloat16)
    outputs = product("hqk,khd->qhd", prob_b, value_rows).astype(jnp.bfloat16)
    attn_b = outputs.reshape(row_total, head_count * VDIM)
    return (
        query_b,
        key_rope,
        latent_unit,
        latent_scale,
        latent_b,
        key_nope,
        value_rows,
        attn_b,
        log_total,
    )


def attention_backward(
    grad_attn_b, normed_b, saved, w_query, w_latent, latent_gain, w_keyval, cosine, sine
):
    (
        query_b,
        key_rope,
        latent_unit,
        latent_scale,
        latent_b,
        key_nope,
        value_rows,
        attn_b,
        log_sums,
    ) = saved
    row_total = normed_b.shape[0]
    head_count = key_nope.shape[1]
    grad_rows = grad_attn_b.reshape(row_total, head_count, VDIM)
    attn_rows = attn_b.reshape(row_total, head_count, VDIM)
    block_rows = score_block()
    scores = masked_scores(query_b, key_nope, key_rope)
    probs = jnp.exp(scores - log_sums)
    prob_b = probs.astype(jnp.bfloat16)
    grad_value = product("hqk,qhd->khd", prob_b, grad_rows)
    grad_probs = product("qhd,khd->hqk", grad_rows, value_rows)
    row_delta = jnp.sum(grad_rows.astype(jnp.float32) * attn_rows.astype(jnp.float32), axis=-1)
    grad_scores = (
        probs * (grad_probs - jnp.transpose(row_delta)[..., None]) * (NOPE + ROPE) ** (-0.5)
    ).astype(jnp.bfloat16)
    grad_query_nope = product("hqk,khd->qhd", grad_scores, key_nope)
    grad_query_rope = product("hqk,kd->qhd", grad_scores, key_rope)
    grad_queries = jnp.concatenate(
        [
            grad_query_nope,
            rotate(
                grad_query_rope, cosine[0:block_rows, None, :], sine[0:block_rows, None, :], -1.0
            ),
        ],
        axis=-1,
    )
    grad_key_nope = product("hqk,qhd->khd", grad_scores, query_b[..., :NOPE])
    grad_key_rope = product("hqk,qhd->kd", grad_scores, query_b[..., NOPE:])
    grad_query_b = grad_queries.reshape(row_total, head_count * (NOPE + ROPE)).astype(jnp.bfloat16)
    grad_keyval_b = (
        jnp.concatenate([grad_key_nope, grad_value], axis=-1)
        .reshape(row_total, head_count * (NOPE + VDIM))
        .astype(jnp.bfloat16)
    )
    grad_query_w = matmul_rows(grad_query_b, normed_b)
    grad_keyval_w = matmul_rows(latent_b, grad_keyval_b)
    grad_latent_normed = matmul_t(grad_keyval_b, w_keyval)
    grad_latent_core, grad_latent_gain = rms_backward(
        grad_latent_normed, latent_unit, latent_scale, latent_gain
    )
    grad_latent_rows = jnp.concatenate(
        [grad_latent_core, rotate(grad_key_rope, cosine, sine, -1.0)], axis=-1
    )
    normed_f = normed_b.astype(jnp.float32)
    grad_latent_w = jnp.dot(grad_latent_rows.T, normed_f, precision=HIGHEST)
    grad_normed = matmul_t(grad_query_b, w_query) + jnp.dot(
        grad_latent_rows, w_latent.astype(jnp.float32).T, precision=HIGHEST
    )
    return (grad_normed, grad_query_w, grad_latent_w, grad_latent_gain, grad_keyval_w)


def shared_forward(normed_b, gate_w, up_w):
    pre_gate = jnp.dot(normed_b, gate_w, preferred_element_type=jnp.float32)
    pre_up = jnp.dot(normed_b, up_w, preferred_element_type=jnp.float32)
    sigma_gate = jax.nn.sigmoid(pre_gate)
    activated = pre_gate * sigma_gate
    return (pre_gate, pre_up, sigma_gate, activated, (activated * pre_up).astype(jnp.bfloat16))


LANES = 128
VMEM_LIMIT = 64000000


def gather_tp(x):
    count = lax.axis_size("tp")
    at = lax.axis_index("tp")
    rows = x.shape[0]
    whole = jnp.zeros((count * rows, x.shape[1]), x.dtype)
    whole = lax.dynamic_update_slice_in_dim(whole, x, at * rows, 0)
    for step in range(1, count):
        came = lax.ppermute(x, "tp", [(i, (i + step) % count) for i in range(count)])
        whole = lax.dynamic_update_slice_in_dim(
            whole, came, ((at + count - step) % count) * rows, 0
        )
    return whole


def exchange_tp(x):
    count = lax.axis_size("tp")
    at = lax.axis_index("tp")
    rows = x.shape[0] // count
    total = lax.dynamic_slice_in_dim(x, at * rows, rows, 0).astype(jnp.float32)
    for step in range(1, count):
        part = lax.dynamic_slice_in_dim(x, ((at + step) % count) * rows, rows, 0)
        came = lax.ppermute(part, "tp", [(i, (i + step) % count) for i in range(count)])
        total = total + came.astype(jnp.float32)
    return total


def gather_wide(x):
    return lax.all_gather(x, "wide", axis=0, tiled=True)


def join_rows(parts):
    total = sum(part.shape[0] for part in parts)
    at = 0
    whole = None
    for part in parts:
        padded = jnp.pad(part, ((at, total - at - part.shape[0]), (0, 0)))
        whole = padded if whole is None else whole + padded
        at += part.shape[0]
    return whole


def scatter_wide_rows(x):
    return lax.psum_scatter(x, "wide", scatter_dimension=0, tiled=True)


def scatter_wide(x):
    return lax.psum_scatter(x, "wide", scatter_dimension=1, tiled=True)


def expert_front_kernel(
    blocks, slots, first_ref, x_ref, c_ref, router_ref, wg_ref, wu_ref, wd_ref,
    g_ref, xs_ref, cs_ref, hidden_ref, pg_ref, pu_ref, pick_ref, back_ref, gate_ref, sums_ref,
):
    f32, bf16 = jnp.float32, jnp.bfloat16
    width = x_ref.shape[1]
    own = x_ref.shape[0] // blocks
    experts = wg_ref.shape[0]
    slot_total = experts * slots
    first = first_ref[0, 0]
    sub = lax.broadcasted_iota(jnp.int32, (LANES, own), 0)
    above = (
        lax.broadcasted_iota(jnp.int32, (own, own), 0)
        < lax.broadcasted_iota(jnp.int32, (own, own), 1)
    ).astype(bf16)
    slot_ids = lax.broadcasted_iota(jnp.int32, (slots, own), 0).astype(f32)
    for b in range(blocks):
        rows = pl.ds(b * own, own)
        x_b = x_ref[rows, :]
        mask = c_ref[rows, width:].astype(f32)
        logits = jnp.dot(x_b, router_ref[...], preferred_element_type=f32)
        chosen = jax.nn.sigmoid(logits) * mask
        gate = ROUTE_SCALE * chosen / jnp.sum(chosen, axis=1, keepdims=True)
        gate_t = gate.T
        mask_t = mask.T
        place_t = jnp.dot(mask_t.astype(bf16), above, preferred_element_type=f32)
        picks = []
        for e in range(experts):
            here = sub == first + e
            mask_row = jnp.sum(jnp.where(here, mask_t, 0.0), axis=0, keepdims=True)
            place_row = jnp.sum(jnp.where(here, place_t, 0.0), axis=0, keepdims=True)
            gate_row = jnp.sum(jnp.where(here, gate_t, 0.0), axis=0, keepdims=True)
            pick = jnp.where(
                (slot_ids == place_row) & (mask_row > 0.0), jnp.ones_like(slot_ids), 0.0
            )
            picks.append(pick)
            gate_ref[e, pl.ds(b * slots, slots), :] = jnp.broadcast_to(
                jnp.sum(pick * gate_row, axis=1, keepdims=True), (slots, LANES)
            )
        pick_all = jnp.concatenate(picks, axis=0)
        pick_b = pick_all.astype(bf16)
        pick_ref[pl.ds(b * slot_total, slot_total), :] = pick_b
        x_s = jnp.dot(pick_b, x_b, preferred_element_type=f32).astype(bf16)
        c_s = jnp.dot(pick_b, c_ref[rows, :width], preferred_element_type=f32).astype(bf16)
        for e in range(experts):
            xs_ref[e, pl.ds(b * slots, slots), :] = x_s[e * slots : (e + 1) * slots]
            cs_ref[e, pl.ds(b * slots, slots), :] = c_s[e * slots : (e + 1) * slots]
    for e in range(experts):
        x_e = xs_ref[e]
        gate = gate_ref[e][:, :1]
        pre_gate = matmul_t(x_e, wg_ref[e])
        pre_up = matmul_t(x_e, wu_ref[e])
        grad_hidden = matmul_t(cs_ref[e], wd_ref[e])
        sigma = jax.nn.sigmoid(pre_gate)
        active = pre_gate * sigma
        hidden = active * pre_up
        sums_ref[e] = jnp.broadcast_to(
            jnp.sum(hidden * grad_hidden, axis=1, keepdims=True), sums_ref.shape[1:]
        )
        hidden_ref[e] = (hidden * gate).astype(bf16)
        weighted = grad_hidden * gate
        grad_pg = (weighted * pre_up * sigma * (1.0 + pre_gate * (1.0 - sigma))).astype(bf16)
        grad_pu = (weighted * active).astype(bf16)
        pg_ref[e] = grad_pg
        pu_ref[e] = grad_pu
        grad_in = (
            jnp.dot(grad_pg, wg_ref[e], preferred_element_type=f32)
            + jnp.dot(grad_pu, wu_ref[e], preferred_element_type=f32)
        ).astype(bf16)
        for b in range(blocks):
            back_ref[b, pl.ds(e * slots, slots), :] = grad_in[b * slots : (b + 1) * slots]
    for b in range(blocks):
        pick = pick_ref[pl.ds(b * slot_total, slot_total), :].astype(f32)
        sums_t = jnp.zeros((LANES, own), f32)
        for e in range(experts):
            row = jnp.sum(
                pick[e * slots : (e + 1) * slots] * sums_ref[e, pl.ds(b * slots, slots), :][:, :1],
                axis=0,
                keepdims=True,
            )
            sums_t = sums_t + jnp.where(sub == first + e, row, 0.0)
        rows = pl.ds(b * own, own)
        g_ref[rows, width:] = sums_t.T.astype(bf16)
        g_ref[rows, :width] = jnp.dot(
            pick.T.astype(bf16), back_ref[b], preferred_element_type=f32
        ).astype(bf16)


def expert_front(first, rows_x, rows_c, router, w_gate, w_up, w_down, blocks, slots, own):
    bf16 = jnp.bfloat16
    total, width = rows_x.shape
    experts, hidden, _ = w_gate.shape
    step_rows = blocks * own
    steps = total // step_rows
    step_slots = blocks * slots
    all_slots = steps * step_slots

    def whole(shape):
        return pl.BlockSpec(shape, lambda i: (0,) * len(shape), pipeline_mode=pl.Buffered(1))

    def per_expert(last):
        return pl.BlockSpec((experts, step_slots, last), lambda i: (0, i, 0))

    flops = 2 * all_slots * experts * width * (5 * hidden + 2 * own) + 2 * total * width * LANES
    return pl.pallas_call(
        lambda *refs: expert_front_kernel(blocks, slots, *refs),
        grid=(steps,),
        in_specs=[
            pl.BlockSpec(memory_space=pltpu.SMEM),
            pl.BlockSpec((step_rows, width), lambda i: (i, 0)),
            pl.BlockSpec((step_rows, width + LANES), lambda i: (i, 0)),
            whole((width, LANES)),
            whole(w_gate.shape),
            whole(w_up.shape),
            whole(w_down.shape),
        ],
        out_specs=[
            pl.BlockSpec((step_rows, width + LANES), lambda i: (i, 0)),
            per_expert(width),
            per_expert(width),
            per_expert(hidden),
            per_expert(hidden),
            per_expert(hidden),
            pl.BlockSpec((blocks * experts * slots, own), lambda i: (i, 0)),
        ],
        out_shape=[
            jax.ShapeDtypeStruct((total, width + LANES), bf16),
            jax.ShapeDtypeStruct((experts, all_slots, width), bf16),
            jax.ShapeDtypeStruct((experts, all_slots, width), bf16),
            jax.ShapeDtypeStruct((experts, all_slots, hidden), bf16),
            jax.ShapeDtypeStruct((experts, all_slots, hidden), bf16),
            jax.ShapeDtypeStruct((experts, all_slots, hidden), bf16),
            jax.ShapeDtypeStruct((total // own * experts * slots, own), bf16),
        ],
        scratch_shapes=[
            pltpu.VMEM((blocks, experts * slots, width), bf16),
            pltpu.VMEM((experts, step_slots, LANES), jnp.float32),
            pltpu.VMEM((experts, step_slots, LANES), jnp.float32),
        ],
        compiler_params=pltpu.CompilerParams(vmem_limit_bytes=VMEM_LIMIT),
        cost_estimate=pl.CostEstimate(
            flops=flops,
            bytes_accessed=2 * width * (3 * total + 2 * experts * all_slots),
            transcendentals=0,
        ),
        name="expert_front",
    )(first, rows_x, rows_c, router, w_gate, w_up, w_down)


def expert_out_kernel(blocks, slots, hidden_ref, pick_ref, wd_ref, y_ref, rows_ref):
    f32, bf16 = jnp.float32, jnp.bfloat16
    experts = wd_ref.shape[0]
    own = y_ref.shape[0] // blocks
    for e in range(experts):
        out = jnp.dot(hidden_ref[e], wd_ref[e], preferred_element_type=f32).astype(bf16)
        for b in range(blocks):
            rows_ref[b, pl.ds(e * slots, slots), :] = out[b * slots : (b + 1) * slots]
    for b in range(blocks):
        pick = pick_ref[pl.ds(b * experts * slots, experts * slots), :].astype(f32)
        y_ref[pl.ds(b * own, own), :] = jnp.dot(
            pick.T.astype(bf16), rows_ref[b], preferred_element_type=f32
        ).astype(bf16)


def expert_out(hidden, picks, w_down, blocks, slots, own):
    bf16 = jnp.bfloat16
    experts, units, width = w_down.shape
    total = picks.shape[0] // (experts * slots) * own
    step_rows = blocks * own
    step_slots = blocks * slots
    steps = total // step_rows
    return pl.pallas_call(
        lambda *refs: expert_out_kernel(blocks, slots, *refs),
        grid=(steps,),
        in_specs=[
            pl.BlockSpec((experts, step_slots, units), lambda i: (0, i, 0)),
            pl.BlockSpec((blocks * experts * slots, own), lambda i: (i, 0)),
            pl.BlockSpec(
                w_down.shape, lambda i: (0, 0, 0), pipeline_mode=pl.Buffered(1)
            ),
        ],
        out_specs=pl.BlockSpec((step_rows, width), lambda i: (i, 0)),
        out_shape=jax.ShapeDtypeStruct((total, width), bf16),
        scratch_shapes=[pltpu.VMEM((blocks, experts * slots, width), bf16)],
        compiler_params=pltpu.CompilerParams(vmem_limit_bytes=VMEM_LIMIT),
        cost_estimate=pl.CostEstimate(
            flops=2 * steps * step_slots * experts * width * (units + own),
            bytes_accessed=2 * total * width,
            transcendentals=0,
        ),
        name="expert_out",
    )(hidden, picks, w_down)


def on_device(
    inputs,
    cotangent,
    expert_choice,
    norm1_gain,
    w_query,
    w_latent,
    latent_gain,
    w_keyval,
    w_out,
    norm2_gain,
    w_router,
    w_shared_gate,
    w_shared_up,
    w_shared_down,
    w_expert_gate,
    w_expert_up,
    w_expert_down,
):
    bf16 = jnp.bfloat16
    f32 = jnp.float32
    tp_count = lax.axis_size("tp")
    wide_count = lax.axis_size("wide")
    wide_at = lax.axis_index("wide")
    own_count, width = inputs.shape
    top_count = expert_choice.shape[1]
    expert_total = w_router.shape[1]
    local_experts = w_expert_gate.shape[0]
    capacity = 8 * (own_count * top_count // (8 * expert_total) + 1)
    slots = -(-capacity // 16) * 16
    seq_rows = own_count * tp_count
    all_rows = seq_rows * wide_count
    blocks = wide_count * tp_count

    chosen_own = jnp.any(
        expert_choice[:, :, None] == jnp.arange(expert_total, dtype=jnp.int32), axis=1
    )
    mask_own = chosen_own.astype(f32)
    input_all = gather_tp(inputs)
    early = jnp.concatenate(
        [cotangent, jnp.pad(mask_own, ((0, 0), (0, LANES - expert_total))).astype(bf16)], axis=1
    )
    input_all, early = lax.optimization_barrier((input_all, early))
    early_seq = gather_tp(early)

    cosine, sine = rotary_tables(seq_rows)
    unit1, _, normed1 = rms_forward(input_all.astype(f32), norm1_gain)
    normed1_b = normed1.astype(bf16)
    saved = attention_forward(normed1_b, w_query, w_latent, latent_gain, w_keyval, cosine, sine)
    attn_part = matmul_t(saved[7], w_out).astype(bf16)
    attn_part, early_seq = lax.optimization_barrier((attn_part, early_seq))
    early_all = gather_wide(early_seq)
    cot_seq = early_seq[:, :width]
    attn_own = exchange_tp(attn_part)
    input_own = inputs.astype(f32)
    hidden_own = input_own + attn_own
    unit2, scale2, normed2 = rms_forward(hidden_own, norm2_gain)
    normed2_own = normed2.astype(bf16)
    normed2_seq = gather_tp(normed2_own)
    gather_from, early_all = lax.optimization_barrier((normed2_seq, early_all))
    normed2_all = gather_wide(gather_from)

    pre_gate, pre_up, sigma_gate, activated, shared_b = shared_forward(
        normed2_seq, w_shared_gate, w_shared_up
    )
    shared_part = matmul_t(shared_b, w_shared_down)
    grad_shared_hidden = jnp.dot(cot_seq, w_shared_down, preferred_element_type=f32)
    grad_pre_gate_b = (
        grad_shared_hidden * pre_up * sigma_gate * (1.0 + pre_gate * (1.0 - sigma_gate))
    ).astype(bf16)
    grad_pre_up_b = (grad_shared_hidden * activated).astype(bf16)
    grad_shared = jnp.concatenate(
        [
            matmul_rows(grad_pre_gate_b, normed2_seq).astype(bf16),
            matmul_rows(grad_pre_up_b, normed2_seq).astype(bf16),
            matmul_rows(shared_b, cot_seq).astype(bf16),
        ],
        axis=0,
    )
    shared_back = matmul_t(grad_pre_gate_b, w_shared_gate) + matmul_t(grad_pre_up_b, w_shared_up)
    first_expert = (wide_at * local_experts).astype(jnp.int32).reshape(1, 1)
    first_expert, shared_part, shared_back, grad_shared = lax.optimization_barrier(
        (first_expert, shared_part, shared_back, grad_shared)
    )
    first = scatter_wide(grad_shared)

    grad_in_all, x_slots, c_slots, hidden_slots, pg_slots, pu_slots, picks = expert_front(
        first_expert,
        normed2_all,
        early_all,
        jnp.pad(w_router, ((0, 0), (0, LANES - expert_total))),
        jnp.swapaxes(w_expert_gate, 1, 2),
        jnp.swapaxes(w_expert_up, 1, 2),
        jnp.swapaxes(w_expert_down, 1, 2),
        tp_count,
        slots,
        own_count,
    )
    grad_in_all, first = lax.optimization_barrier((grad_in_all, first))
    first = first.astype(f32)
    grad_in_seq = scatter_wide_rows(grad_in_all)
    out_all = expert_out(
        hidden_slots, picks, jnp.swapaxes(w_expert_down, 1, 2), tp_count, slots, own_count
    )
    out_seq = scatter_wide_rows(out_all)
    grad_expert_gate = product("emd,emf->edf", x_slots, pg_slots)
    grad_expert_up = product("emd,emf->edf", x_slots, pu_slots)
    grad_expert_down = product("emd,emf->edf", c_slots, hidden_slots)
    grad_in_seq, grad_expert_gate, grad_expert_up, grad_expert_down = lax.optimization_barrier(
        (grad_in_seq, grad_expert_gate, grad_expert_up, grad_expert_down)
    )

    back = (
        grad_in_seq.astype(f32) + jnp.pad(shared_back, ((0, 0), (0, LANES)))
    ).astype(bf16)
    back_own = exchange_tp(back)
    grad_gate = back_own[:, width : width + expert_total]
    logits = jnp.dot(normed2_own, w_router, preferred_element_type=f32)
    selected = jax.nn.sigmoid(logits)
    sel_total = jnp.sum(selected * mask_own, axis=1, keepdims=True)
    weighted = jnp.sum(grad_gate * selected * mask_own, axis=1, keepdims=True)
    grad_selected = ROUTE_SCALE * (grad_gate / sel_total - weighted / (sel_total * sel_total))
    grad_logits = grad_selected * selected * (1.0 - selected) * mask_own
    grad_router = jnp.dot(grad_logits.T, normed2_own.astype(f32), precision=HIGHEST)
    grad_normed2 = back_own[:, :width] + jnp.dot(
        grad_logits, w_router.astype(f32).T, precision=HIGHEST
    )
    grad_h2, grad_g2 = rms_backward(grad_normed2, unit2, scale2, norm2_gain)
    grad_hidden_own = cotangent.astype(f32) + grad_h2
    grad_hidden_b = gather_tp(grad_hidden_own.astype(bf16))

    grad_wo = matmul_rows(saved[7], grad_hidden_b).astype(bf16)
    grad_attn_b = jnp.dot(grad_hidden_b, w_out, preferred_element_type=f32).astype(bf16)
    grad_normed1, grad_wq, grad_wlat, grad_lgain, grad_wkv = attention_backward(
        grad_attn_b, normed1_b, saved, w_query, w_latent, latent_gain, w_keyval, cosine, sine
    )
    grad_g1 = jnp.sum(grad_normed1 * unit1, axis=0)
    grad_normed1_own = exchange_tp(grad_normed1.astype(bf16))
    scaled = grad_normed1_own * norm1_gain
    unit1_own, scale1_own, _ = rms_forward(input_own, norm1_gain)
    grad_input = grad_hidden_own + scale1_own * (
        scaled - unit1_own * jnp.mean(scaled * unit1_own, axis=-1, keepdims=True)
    )

    output = hidden_own + exchange_tp((out_seq.astype(f32) + shared_part).astype(bf16))
    chunk = width // wide_count
    shared_width = shared_b.shape[1]
    rank = latent_gain.shape[0]
    gain_rows = rank // blocks
    lgain_row = jnp.pad(
        grad_lgain.reshape(blocks, gain_rows), ((0, 0), (0, width // blocks - gain_rows))
    ).reshape(1, width)
    latent_count = grad_wlat.shape[0]
    s0 = latent_count + expert_total
    gains = jnp.concatenate(
        [grad_g1[None], grad_g2[None], lgain_row, jnp.zeros((13, width), f32)], axis=0
    )
    rank_rows = rank // wide_count
    groups = grad_wkv.shape[1] // chunk
    folded = (
        grad_wkv.astype(bf16)
        .reshape(wide_count, rank_rows, groups, chunk)
        .transpose(2, 1, 0, 3)
        .reshape(groups * rank_rows, width)
    )
    second = scatter_wide(
        join_rows(
            [
                grad_wo,
                grad_wq.astype(bf16),
                folded,
                grad_wlat.astype(bf16),
                grad_router.astype(bf16),
                gains.astype(bf16),
            ]
        )
    )
    c0 = grad_wo.shape[0]
    c1 = c0 + grad_wq.shape[0]
    c2 = c1 + groups * rank_rows
    out_wo = second[:c0].astype(f32).T
    out_wq = second[c0:c1].astype(f32).T
    out_wkv = (
        second[c1:c2]
        .reshape(groups, rank_rows, chunk)
        .transpose(1, 0, 2)
        .reshape(rank_rows, grad_wkv.shape[1])
        .astype(f32)
    )
    small_own = exchange_tp(second[c2:].T)
    return (
        output,
        grad_input,
        small_own[:, s0],
        out_wq,
        small_own[:, :latent_count],
        small_own[:gain_rows, s0 + 2],
        out_wkv,
        out_wo,
        small_own[:, s0 + 1],
        small_own[:, latent_count:s0],
        first[:shared_width].T,
        first[shared_width : 2 * shared_width].T,
        first[2 * shared_width :].T,
        grad_expert_gate,
        grad_expert_up,
        grad_expert_down,
    )


def solution(mesh):
    in_specs = (
        P(("wide", "tp"), None),
        P(("wide", "tp"), None),
        P(("wide", "tp"), None),
        P(),
        P(None, "tp"),
        P(),
        P(),
        P(None, "tp"),
        P(None, "tp"),
        P(),
        P(),
        P(None, "tp"),
        P(None, "tp"),
        P(None, "tp"),
        P("wide", None, "tp"),
        P("wide", None, "tp"),
        P("wide", None, "tp"),
    )
    out_specs = (
        P(("wide", "tp"), None),
        P(("wide", "tp"), None),
        P(("wide", "tp")),
        P("wide", "tp"),
        P(("wide", "tp"), None),
        P(("wide", "tp")),
        P("wide", "tp"),
        P("wide", "tp"),
        P(("wide", "tp")),
        P(("wide", "tp"), None),
        P("wide", "tp"),
        P("wide", "tp"),
        P("wide", "tp"),
        P("wide", None, "tp"),
        P("wide", None, "tp"),
        P("wide", None, "tp"),
    )
    return jax.shard_map(
        on_device, mesh=mesh, in_specs=in_specs, out_specs=out_specs, check_vma=False
    )
```

```python
import jax
import jax.numpy as jnp
from jax import lax
from jax.experimental import pallas as pl
from jax.experimental.pallas import tpu as pltpu
from jax.sharding import PartitionSpec as P

NOPE = 128
ROPE = 64
VDIM = 128
RANK = 512


EPSILON = 1e-06
ROUTE_SCALE = 2.446
THETA = 50000.0
HIGHEST = lax.Precision.HIGHEST


def product(form, left, right):
    return jnp.einsum(form, left, right, preferred_element_type=jnp.float32)


def matmul_t(left, right):
    return lax.dot_general(
        left, right, (((1,), (1,)), ((), ())), preferred_element_type=jnp.float32
    )


def matmul_rows(left, right):
    return lax.dot_general(
        left, right, (((0,), (0,)), ((), ())), preferred_element_type=jnp.float32
    )


def rotary_tables(positions):
    half_width = ROPE // 2
    position = jnp.arange(positions, dtype=jnp.float32)[:, None]
    inverse = THETA ** (-jnp.arange(half_width, dtype=jnp.float32) / half_width)
    angle = position * inverse[None, :]
    return (jnp.cos(angle), jnp.sin(angle))


def rotate(vector, cosine, sine, turn):
    half_width = vector.shape[-1] // 2
    lower = vector[..., :half_width]
    upper = vector[..., half_width:]
    return jnp.concatenate(
        [lower * cosine - turn * upper * sine, upper * cosine + turn * lower * sine], axis=-1
    )


def rms_forward(vector, gain_vector):
    inv_scale = lax.rsqrt(jnp.mean(vector * vector, axis=-1, keepdims=True) + EPSILON)
    unit_rows = vector * inv_scale
    return (unit_rows, inv_scale, unit_rows * gain_vector)


def rms_backward(grad_normed, unit_rows, inv_scale, gain_vector):
    scaled = grad_normed * gain_vector
    grad_in = inv_scale * (
        scaled - unit_rows * jnp.mean(scaled * unit_rows, axis=-1, keepdims=True)
    )
    return (grad_in, jnp.sum(grad_normed * unit_rows, axis=0))


def score_block():
    return 512


def masked_scores(query_block, key_nope, key_rope):
    query_total = query_block.shape[0]
    key_total = key_nope.shape[0]
    scores = product("qhd,khd->hqk", query_block[..., :NOPE], key_nope)
    scores = scores + product("qhd,kd->hqk", query_block[..., NOPE:], key_rope)
    scores = scores * (NOPE + ROPE) ** (-0.5)
    query_pos = jnp.arange(query_total, dtype=jnp.int32)[:, None]
    key_pos = jnp.arange(key_total, dtype=jnp.int32)[None, :]
    return jnp.where((key_pos <= query_pos)[None], scores, -1e30)


def attention_forward(normed_b, w_query, w_latent, latent_gain, w_keyval, cosine, sine):
    row_total = normed_b.shape[0]
    head_count = w_keyval.shape[1] // (NOPE + VDIM)
    query_full = jnp.dot(normed_b, w_query, preferred_element_type=jnp.float32).reshape(
        row_total, head_count, NOPE + ROPE
    )
    query_b = jnp.concatenate(
        [
            query_full[..., :NOPE],
            rotate(query_full[..., NOPE:], cosine[:, None, :], sine[:, None, :], 1.0),
        ],
        axis=-1,
    ).astype(jnp.bfloat16)
    latent = jnp.dot(normed_b, w_latent, preferred_element_type=jnp.float32)
    key_rope = rotate(latent[:, RANK:], cosine, sine, 1.0).astype(jnp.bfloat16)
    latent_unit, latent_scale, latent_normed = rms_forward(latent[:, :RANK], latent_gain)
    latent_b = latent_normed.astype(jnp.bfloat16)
    keyval = (
        jnp.dot(latent_b, w_keyval, preferred_element_type=jnp.float32)
        .reshape(row_total, head_count, NOPE + VDIM)
        .astype(jnp.bfloat16)
    )
    key_nope = keyval[..., :NOPE]
    value_rows = keyval[..., NOPE:]
    scores = masked_scores(query_b, key_nope, key_rope)
    row_max = jnp.max(scores, axis=-1, keepdims=True)
    log_total = row_max + jnp.log(jnp.sum(jnp.exp(scores - row_max), axis=-1, keepdims=True))
    prob_b = jnp.exp(scores - log_total).astype(jnp.bfloat16)
    outputs = product("hqk,khd->qhd", prob_b, value_rows).astype(jnp.bfloat16)
    attn_b = outputs.reshape(row_total, head_count * VDIM)
    return (
        query_b,
        key_rope,
        latent_unit,
        latent_scale,
        latent_b,
        key_nope,
        value_rows,
        attn_b,
        log_total,
    )


def attention_backward(
    grad_attn_b, normed_b, saved, w_query, w_latent, latent_gain, w_keyval, cosine, sine
):
    (
        query_b,
        key_rope,
        latent_unit,
        latent_scale,
        latent_b,
        key_nope,
        value_rows,
        attn_b,
        log_sums,
    ) = saved
    row_total = normed_b.shape[0]
    head_count = key_nope.shape[1]
    grad_rows = grad_attn_b.reshape(row_total, head_count, VDIM)
    attn_rows = attn_b.reshape(row_total, head_count, VDIM)
    block_rows = score_block()
    scores = masked_scores(query_b, key_nope, key_rope)
    probs = jnp.exp(scores - log_sums)
    prob_b = probs.astype(jnp.bfloat16)
    grad_value = product("hqk,qhd->khd", prob_b, grad_rows)
    grad_probs = product("qhd,khd->hqk", grad_rows, value_rows)
    row_delta = jnp.sum(grad_rows.astype(jnp.float32) * attn_rows.astype(jnp.float32), axis=-1)
    grad_scores = (
        probs * (grad_probs - jnp.transpose(row_delta)[..., None]) * (NOPE + ROPE) ** (-0.5)
    ).astype(jnp.bfloat16)
    grad_query_nope = product("hqk,khd->qhd", grad_scores, key_nope)
    grad_query_rope = product("hqk,kd->qhd", grad_scores, key_rope)
    grad_queries = jnp.concatenate(
        [
            grad_query_nope,
            rotate(
                grad_query_rope, cosine[0:block_rows, None, :], sine[0:block_rows, None, :], -1.0
            ),
        ],
        axis=-1,
    )
    grad_key_nope = product("hqk,qhd->khd", grad_scores, query_b[..., :NOPE])
    grad_key_rope = product("hqk,qhd->kd", grad_scores, query_b[..., NOPE:])
    grad_query_b = grad_queries.reshape(row_total, head_count * (NOPE + ROPE)).astype(jnp.bfloat16)
    grad_keyval_b = (
        jnp.concatenate([grad_key_nope, grad_value], axis=-1)
        .reshape(row_total, head_count * (NOPE + VDIM))
        .astype(jnp.bfloat16)
    )
    grad_query_w = matmul_rows(grad_query_b, normed_b)
    grad_keyval_w = matmul_rows(latent_b, grad_keyval_b)
    grad_latent_normed = matmul_t(grad_keyval_b, w_keyval)
    grad_latent_core, grad_latent_gain = rms_backward(
        grad_latent_normed, latent_unit, latent_scale, latent_gain
    )
    grad_latent_rows = jnp.concatenate(
        [grad_latent_core, rotate(grad_key_rope, cosine, sine, -1.0)], axis=-1
    )
    normed_f = normed_b.astype(jnp.float32)
    grad_latent_w = jnp.dot(grad_latent_rows.T, normed_f, precision=HIGHEST)
    grad_normed = matmul_t(grad_query_b, w_query) + jnp.dot(
        grad_latent_rows, w_latent.astype(jnp.float32).T, precision=HIGHEST
    )
    return (grad_normed, grad_query_w, grad_latent_w, grad_latent_gain, grad_keyval_w)


def shared_forward(normed_b, gate_w, up_w):
    pre_gate = jnp.dot(normed_b, gate_w, preferred_element_type=jnp.float32)
    pre_up = jnp.dot(normed_b, up_w, preferred_element_type=jnp.float32)
    sigma_gate = jax.nn.sigmoid(pre_gate)
    activated = pre_gate * sigma_gate
    return (pre_gate, pre_up, sigma_gate, activated, (activated * pre_up).astype(jnp.bfloat16))


LANES = 128
VMEM_LIMIT = 64000000


def gather_tp(x):
    count = lax.axis_size("tp")
    at = lax.axis_index("tp")
    rows = x.shape[0]
    whole = jnp.zeros((count * rows, x.shape[1]), x.dtype)
    whole = lax.dynamic_update_slice_in_dim(whole, x, at * rows, 0)
    for step in range(1, count):
        came = lax.ppermute(x, "tp", [(i, (i + step) % count) for i in range(count)])
        whole = lax.dynamic_update_slice_in_dim(
            whole, came, ((at + count - step) % count) * rows, 0
        )
    return whole


def exchange_tp(x):
    count = lax.axis_size("tp")
    at = lax.axis_index("tp")
    rows = x.shape[0] // count
    total = lax.dynamic_slice_in_dim(x, at * rows, rows, 0).astype(jnp.float32)
    for step in range(1, count):
        part = lax.dynamic_slice_in_dim(x, ((at + step) % count) * rows, rows, 0)
        came = lax.ppermute(part, "tp", [(i, (i + step) % count) for i in range(count)])
        total = total + came.astype(jnp.float32)
    return total


def gather_wide(x):
    return lax.all_gather(x, "wide", axis=0, tiled=True)


def fold_pieces(pieces, bit, count):
    sent = [r for r in sorted(pieces) if r & bit]
    chunk = pieces[sent[0]].shape[1]
    came = lax.ppermute(
        jnp.concatenate([pieces[r] for r in sent], axis=1),
        "wide",
        [(i, i ^ bit) for i in range(count)],
    )
    kept = {}
    for place, r in enumerate(sent):
        part = came[:, place * chunk : (place + 1) * chunk].astype(jnp.float32)
        kept[r ^ bit] = (pieces[r ^ bit].astype(jnp.float32) + part).astype(jnp.bfloat16)
    return kept


def halve_wide(x):
    count = lax.axis_size("wide")
    at = lax.axis_index("wide")
    chunk = x.shape[1] // count
    pieces = {
        r: lax.dynamic_slice_in_dim(x, (at ^ r) * chunk, chunk, 1) for r in range(count)
    }
    bits = [1 << b for b in range(count.bit_length() - 1)]
    pieces = fold_pieces(pieces, bits[0], count)
    half = x.shape[0] // 32 * 16
    done = []
    for rows, order in ((slice(0, half), bits[1:]), (slice(half, None), bits[:0:-1])):
        part = {r: piece[rows] for r, piece in pieces.items()}
        for bit in order:
            part = fold_pieces(part, bit, count)
        done.append(part[0])
    return jnp.concatenate(done, axis=0)


def join_rows(parts):
    total = sum(part.shape[0] for part in parts)
    at = 0
    whole = None
    for part in parts:
        padded = jnp.pad(part, ((at, total - at - part.shape[0]), (0, 0)))
        whole = padded if whole is None else whole + padded
        at += part.shape[0]
    return whole


def scatter_wide_rows(x):
    return lax.psum_scatter(x, "wide", scatter_dimension=0, tiled=True)


def scatter_wide(x):
    return lax.psum_scatter(x, "wide", scatter_dimension=1, tiled=True)


def expert_front_kernel(
    blocks, slots, first_ref, x_ref, c_ref, router_ref, wg_ref, wu_ref, wd_ref,
    g_ref, xs_ref, cs_ref, hidden_ref, pg_ref, pu_ref, pick_ref, back_ref, gate_ref, sums_ref,
):
    f32, bf16 = jnp.float32, jnp.bfloat16
    width = x_ref.shape[1]
    own = x_ref.shape[0] // blocks
    experts = wg_ref.shape[0]
    slot_total = experts * slots
    first = first_ref[0, 0]
    sub = lax.broadcasted_iota(jnp.int32, (LANES, own), 0)
    above = (
        lax.broadcasted_iota(jnp.int32, (own, own), 0)
        < lax.broadcasted_iota(jnp.int32, (own, own), 1)
    ).astype(bf16)
    slot_ids = lax.broadcasted_iota(jnp.int32, (slots, own), 0).astype(f32)
    for b in range(blocks):
        rows = pl.ds(b * own, own)
        x_b = x_ref[rows, :]
        mask = c_ref[rows, width:].astype(f32)
        logits = jnp.dot(x_b, router_ref[...], preferred_element_type=f32)
        chosen = jax.nn.sigmoid(logits) * mask
        gate = ROUTE_SCALE * chosen / jnp.sum(chosen, axis=1, keepdims=True)
        gate_t = gate.T
        mask_t = mask.T
        place_t = jnp.dot(mask_t.astype(bf16), above, preferred_element_type=f32)
        picks = []
        for e in range(experts):
            here = sub == first + e
            mask_row = jnp.sum(jnp.where(here, mask_t, 0.0), axis=0, keepdims=True)
            place_row = jnp.sum(jnp.where(here, place_t, 0.0), axis=0, keepdims=True)
            gate_row = jnp.sum(jnp.where(here, gate_t, 0.0), axis=0, keepdims=True)
            pick = jnp.where(
                (slot_ids == place_row) & (mask_row > 0.0), jnp.ones_like(slot_ids), 0.0
            )
            picks.append(pick)
            gate_ref[e, pl.ds(b * slots, slots), :] = jnp.broadcast_to(
                jnp.sum(pick * gate_row, axis=1, keepdims=True), (slots, LANES)
            )
        pick_all = jnp.concatenate(picks, axis=0)
        pick_b = pick_all.astype(bf16)
        pick_ref[pl.ds(b * slot_total, slot_total), :] = pick_b
        x_s = jnp.dot(pick_b, x_b, preferred_element_type=f32).astype(bf16)
        c_s = jnp.dot(pick_b, c_ref[rows, :width], preferred_element_type=f32).astype(bf16)
        for e in range(experts):
            xs_ref[e, pl.ds(b * slots, slots), :] = x_s[e * slots : (e + 1) * slots]
            cs_ref[e, pl.ds(b * slots, slots), :] = c_s[e * slots : (e + 1) * slots]
    for e in range(experts):
        x_e = xs_ref[e]
        gate = gate_ref[e][:, :1]
        pre_gate = matmul_t(x_e, wg_ref[e])
        pre_up = matmul_t(x_e, wu_ref[e])
        grad_hidden = matmul_t(cs_ref[e], wd_ref[e])
        sigma = jax.nn.sigmoid(pre_gate)
        active = pre_gate * sigma
        hidden = active * pre_up
        sums_ref[e] = jnp.broadcast_to(
            jnp.sum(hidden * grad_hidden, axis=1, keepdims=True), sums_ref.shape[1:]
        )
        hidden_ref[e] = (hidden * gate).astype(bf16)
        weighted = grad_hidden * gate
        grad_pg = (weighted * pre_up * sigma * (1.0 + pre_gate * (1.0 - sigma))).astype(bf16)
        grad_pu = (weighted * active).astype(bf16)
        pg_ref[e] = grad_pg
        pu_ref[e] = grad_pu
        grad_in = (
            jnp.dot(grad_pg, wg_ref[e], preferred_element_type=f32)
            + jnp.dot(grad_pu, wu_ref[e], preferred_element_type=f32)
        ).astype(bf16)
        for b in range(blocks):
            back_ref[b, pl.ds(e * slots, slots), :] = grad_in[b * slots : (b + 1) * slots]
    for b in range(blocks):
        pick = pick_ref[pl.ds(b * slot_total, slot_total), :].astype(f32)
        sums_t = jnp.zeros((LANES, own), f32)
        for e in range(experts):
            row = jnp.sum(
                pick[e * slots : (e + 1) * slots] * sums_ref[e, pl.ds(b * slots, slots), :][:, :1],
                axis=0,
                keepdims=True,
            )
            sums_t = sums_t + jnp.where(sub == first + e, row, 0.0)
        rows = pl.ds(b * own, own)
        g_ref[rows, width:] = sums_t.T.astype(bf16)
        g_ref[rows, :width] = jnp.dot(
            pick.T.astype(bf16), back_ref[b], preferred_element_type=f32
        ).astype(bf16)


def expert_front(first, rows_x, rows_c, router, w_gate, w_up, w_down, blocks, slots, own):
    bf16 = jnp.bfloat16
    total, width = rows_x.shape
    experts, hidden, _ = w_gate.shape
    step_rows = blocks * own
    steps = total // step_rows
    step_slots = blocks * slots
    all_slots = steps * step_slots

    def whole(shape):
        return pl.BlockSpec(shape, lambda i: (0,) * len(shape), pipeline_mode=pl.Buffered(1))

    def per_expert(last):
        return pl.BlockSpec((experts, step_slots, last), lambda i: (0, i, 0))

    flops = 2 * all_slots * experts * width * (5 * hidden + 2 * own) + 2 * total * width * LANES
    return pl.pallas_call(
        lambda *refs: expert_front_kernel(blocks, slots, *refs),
        grid=(steps,),
        in_specs=[
            pl.BlockSpec(memory_space=pltpu.SMEM),
            pl.BlockSpec((step_rows, width), lambda i: (i, 0)),
            pl.BlockSpec((step_rows, width + LANES), lambda i: (i, 0)),
            whole((width, LANES)),
            whole(w_gate.shape),
            whole(w_up.shape),
            whole(w_down.shape),
        ],
        out_specs=[
            pl.BlockSpec((step_rows, width + LANES), lambda i: (i, 0)),
            per_expert(width),
            per_expert(width),
            per_expert(hidden),
            per_expert(hidden),
            per_expert(hidden),
            pl.BlockSpec((blocks * experts * slots, own), lambda i: (i, 0)),
        ],
        out_shape=[
            jax.ShapeDtypeStruct((total, width + LANES), bf16),
            jax.ShapeDtypeStruct((experts, all_slots, width), bf16),
            jax.ShapeDtypeStruct((experts, all_slots, width), bf16),
            jax.ShapeDtypeStruct((experts, all_slots, hidden), bf16),
            jax.ShapeDtypeStruct((experts, all_slots, hidden), bf16),
            jax.ShapeDtypeStruct((experts, all_slots, hidden), bf16),
            jax.ShapeDtypeStruct((total // own * experts * slots, own), bf16),
        ],
        scratch_shapes=[
            pltpu.VMEM((blocks, experts * slots, width), bf16),
            pltpu.VMEM((experts, step_slots, LANES), jnp.float32),
            pltpu.VMEM((experts, step_slots, LANES), jnp.float32),
        ],
        compiler_params=pltpu.CompilerParams(vmem_limit_bytes=VMEM_LIMIT),
        cost_estimate=pl.CostEstimate(
            flops=flops,
            bytes_accessed=2 * width * (3 * total + 2 * experts * all_slots),
            transcendentals=0,
        ),
        name="expert_front",
    )(first, rows_x, rows_c, router, w_gate, w_up, w_down)


def expert_out_kernel(blocks, slots, hidden_ref, pick_ref, wd_ref, y_ref, rows_ref):
    f32, bf16 = jnp.float32, jnp.bfloat16
    experts = wd_ref.shape[0]
    own = y_ref.shape[0] // blocks
    for e in range(experts):
        out = jnp.dot(hidden_ref[e], wd_ref[e], preferred_element_type=f32).astype(bf16)
        for b in range(blocks):
            rows_ref[b, pl.ds(e * slots, slots), :] = out[b * slots : (b + 1) * slots]
    for b in range(blocks):
        pick = pick_ref[pl.ds(b * experts * slots, experts * slots), :].astype(f32)
        y_ref[pl.ds(b * own, own), :] = jnp.dot(
            pick.T.astype(bf16), rows_ref[b], preferred_element_type=f32
        ).astype(bf16)


def expert_out(hidden, picks, w_down, blocks, slots, own):
    bf16 = jnp.bfloat16
    experts, units, width = w_down.shape
    total = picks.shape[0] // (experts * slots) * own
    step_rows = blocks * own
    step_slots = blocks * slots
    steps = total // step_rows
    return pl.pallas_call(
        lambda *refs: expert_out_kernel(blocks, slots, *refs),
        grid=(steps,),
        in_specs=[
            pl.BlockSpec((experts, step_slots, units), lambda i: (0, i, 0)),
            pl.BlockSpec((blocks * experts * slots, own), lambda i: (i, 0)),
            pl.BlockSpec(
                w_down.shape, lambda i: (0, 0, 0), pipeline_mode=pl.Buffered(1)
            ),
        ],
        out_specs=pl.BlockSpec((step_rows, width), lambda i: (i, 0)),
        out_shape=jax.ShapeDtypeStruct((total, width), bf16),
        scratch_shapes=[pltpu.VMEM((blocks, experts * slots, width), bf16)],
        compiler_params=pltpu.CompilerParams(vmem_limit_bytes=VMEM_LIMIT),
        cost_estimate=pl.CostEstimate(
            flops=2 * steps * step_slots * experts * width * (units + own),
            bytes_accessed=2 * total * width,
            transcendentals=0,
        ),
        name="expert_out",
    )(hidden, picks, w_down)


def on_device(
    inputs,
    cotangent,
    expert_choice,
    norm1_gain,
    w_query,
    w_latent,
    latent_gain,
    w_keyval,
    w_out,
    norm2_gain,
    w_router,
    w_shared_gate,
    w_shared_up,
    w_shared_down,
    w_expert_gate,
    w_expert_up,
    w_expert_down,
):
    bf16 = jnp.bfloat16
    f32 = jnp.float32
    tp_count = lax.axis_size("tp")
    wide_count = lax.axis_size("wide")
    wide_at = lax.axis_index("wide")
    own_count, width = inputs.shape
    top_count = expert_choice.shape[1]
    expert_total = w_router.shape[1]
    local_experts = w_expert_gate.shape[0]
    capacity = 8 * (own_count * top_count // (8 * expert_total) + 1)
    slots = -(-capacity // 16) * 16
    seq_rows = own_count * tp_count
    all_rows = seq_rows * wide_count
    blocks = wide_count * tp_count

    chosen_own = jnp.any(
        expert_choice[:, :, None] == jnp.arange(expert_total, dtype=jnp.int32), axis=1
    )
    mask_own = chosen_own.astype(f32)
    input_all = gather_tp(inputs)
    early = jnp.concatenate(
        [cotangent, jnp.pad(mask_own, ((0, 0), (0, LANES - expert_total))).astype(bf16)], axis=1
    )
    input_all, early = lax.optimization_barrier((input_all, early))
    early_seq = gather_tp(early)

    cosine, sine = rotary_tables(seq_rows)
    unit1, _, normed1 = rms_forward(input_all.astype(f32), norm1_gain)
    normed1_b = normed1.astype(bf16)
    saved = attention_forward(normed1_b, w_query, w_latent, latent_gain, w_keyval, cosine, sine)
    attn_part = matmul_t(saved[7], w_out).astype(bf16)
    attn_part, early_seq = lax.optimization_barrier((attn_part, early_seq))
    half = seq_rows // 2
    early_parts = [gather_wide(early_seq[:half]), gather_wide(early_seq[half:])]
    cot_seq = early_seq[:, :width]
    attn_own = exchange_tp(attn_part)
    input_own = inputs.astype(f32)
    hidden_own = input_own + attn_own
    unit2, scale2, normed2 = rms_forward(hidden_own, norm2_gain)
    normed2_own = normed2.astype(bf16)
    normed2_seq = gather_tp(normed2_own)
    gather_from, early_parts = lax.optimization_barrier((normed2_seq, early_parts))
    normed2_parts = [gather_wide(gather_from[:half])]
    rest = gather_from[half:]

    pre_gate, pre_up, sigma_gate, activated, shared_b = shared_forward(
        normed2_seq, w_shared_gate, w_shared_up
    )
    shared_part = matmul_t(shared_b, w_shared_down)
    grad_shared_hidden = jnp.dot(cot_seq, w_shared_down, preferred_element_type=f32)
    grad_pre_gate_b = (
        grad_shared_hidden * pre_up * sigma_gate * (1.0 + pre_gate * (1.0 - sigma_gate))
    ).astype(bf16)
    grad_pre_up_b = (grad_shared_hidden * activated).astype(bf16)
    grad_shared = jnp.concatenate(
        [
            matmul_rows(grad_pre_gate_b, normed2_seq).astype(bf16),
            matmul_rows(grad_pre_up_b, normed2_seq).astype(bf16),
            matmul_rows(shared_b, cot_seq).astype(bf16),
        ],
        axis=0,
    )
    shared_back = matmul_t(grad_pre_gate_b, w_shared_gate) + matmul_t(grad_pre_up_b, w_shared_up)
    first_expert = (wide_at * local_experts).astype(jnp.int32).reshape(1, 1)
    rest, first_expert, normed2_parts, shared_part, shared_back, grad_shared = (
        lax.optimization_barrier(
            (rest, first_expert, normed2_parts, shared_part, shared_back, grad_shared)
        )
    )
    normed2_parts.append(gather_wide(rest))

    weights_t = [jnp.swapaxes(w, 1, 2) for w in (w_expert_gate, w_expert_up, w_expert_down)]
    router = jnp.pad(w_router, ((0, 0), (0, LANES - expert_total)))
    fronts, grad_in_parts = [], []
    for rows_x, rows_c in zip(normed2_parts, early_parts):
        front = expert_front(
            first_expert, rows_x, rows_c, router, *weights_t, tp_count, slots, own_count
        )
        fronts.append(front[1:])
        grad_in_parts.append(scatter_wide_rows(front[0]))
    x_slots, c_slots, hidden_slots, pg_slots, pu_slots = (
        [front[at] for front in fronts] for at in range(5)
    )
    out_all = jnp.concatenate(
        [
            expert_out(
                front[2], front[5], weights_t[2], tp_count, slots, own_count
            ).reshape(wide_count, half, width)
            for front in fronts
        ],
        axis=1,
    ).reshape(all_rows, width)

    def over_slots(left, right):
        return sum(product("emd,emf->edf", a, b) for a, b in zip(left, right))

    grad_expert_gate = over_slots(x_slots, pg_slots)
    grad_expert_up = over_slots(x_slots, pu_slots)
    grad_expert_down = over_slots(c_slots, hidden_slots)
    grad_in_seq = jnp.concatenate(grad_in_parts, axis=0)
    grad_in_seq, grad_expert_gate, grad_expert_up, grad_expert_down, grad_shared, out_all = (
        lax.optimization_barrier(
            (grad_in_seq, grad_expert_gate, grad_expert_up, grad_expert_down, grad_shared, out_all)
        )
    )
    out_seq = scatter_wide_rows(out_all)
    first = halve_wide(grad_shared)

    back = (
        grad_in_seq.astype(f32) + jnp.pad(shared_back, ((0, 0), (0, LANES)))
    ).astype(bf16)
    back_own = exchange_tp(back)
    grad_gate = back_own[:, width : width + expert_total]
    logits = jnp.dot(normed2_own, w_router, preferred_element_type=f32)
    selected = jax.nn.sigmoid(logits)
    sel_total = jnp.sum(selected * mask_own, axis=1, keepdims=True)
    weighted = jnp.sum(grad_gate * selected * mask_own, axis=1, keepdims=True)
    grad_selected = ROUTE_SCALE * (grad_gate / sel_total - weighted / (sel_total * sel_total))
    grad_logits = grad_selected * selected * (1.0 - selected) * mask_own
    grad_router = jnp.dot(grad_logits.T, normed2_own.astype(f32), precision=HIGHEST)
    grad_normed2 = back_own[:, :width] + jnp.dot(
        grad_logits, w_router.astype(f32).T, precision=HIGHEST
    )
    grad_h2, grad_g2 = rms_backward(grad_normed2, unit2, scale2, norm2_gain)
    grad_hidden_own = cotangent.astype(f32) + grad_h2
    grad_hidden_b = gather_tp(grad_hidden_own.astype(bf16))

    grad_wo = matmul_rows(saved[7], grad_hidden_b).astype(bf16)
    grad_attn_b = jnp.dot(grad_hidden_b, w_out, preferred_element_type=f32).astype(bf16)
    grad_normed1, grad_wq, grad_wlat, grad_lgain, grad_wkv = attention_backward(
        grad_attn_b, normed1_b, saved, w_query, w_latent, latent_gain, w_keyval, cosine, sine
    )
    grad_g1 = jnp.sum(grad_normed1 * unit1, axis=0)
    grad_normed1_own = exchange_tp(grad_normed1.astype(bf16))
    scaled = grad_normed1_own * norm1_gain
    unit1_own, scale1_own, _ = rms_forward(input_own, norm1_gain)
    grad_input = grad_hidden_own + scale1_own * (
        scaled - unit1_own * jnp.mean(scaled * unit1_own, axis=-1, keepdims=True)
    )

    chunk = width // wide_count
    shared_width = shared_b.shape[1]
    rank = latent_gain.shape[0]
    gain_rows = rank // blocks
    lgain_row = jnp.pad(
        grad_lgain.reshape(blocks, gain_rows), ((0, 0), (0, width // blocks - gain_rows))
    ).reshape(1, width)
    latent_count = grad_wlat.shape[0]
    s0 = latent_count + expert_total
    gains = jnp.concatenate(
        [grad_g1[None], grad_g2[None], lgain_row, jnp.zeros((13, width), f32)], axis=0
    )
    rank_rows = rank // wide_count
    groups = grad_wkv.shape[1] // chunk
    folded = (
        grad_wkv.astype(bf16)
        .reshape(wide_count, rank_rows, groups, chunk)
        .transpose(2, 1, 0, 3)
        .reshape(groups * rank_rows, width)
    )
    joined = join_rows(
        [
            grad_wo,
            grad_wq.astype(bf16),
            folded,
            grad_wlat.astype(bf16),
            grad_router.astype(bf16),
            gains.astype(bf16),
        ]
    )
    joined, out_seq, first = lax.optimization_barrier((joined, out_seq, first))
    first = first.astype(f32)
    second = scatter_wide(joined)
    output = hidden_own + exchange_tp((out_seq.astype(f32) + shared_part).astype(bf16))
    c0 = grad_wo.shape[0]
    c1 = c0 + grad_wq.shape[0]
    c2 = c1 + groups * rank_rows
    out_wo = second[:c0].astype(f32).T
    out_wq = second[c0:c1].astype(f32).T
    out_wkv = (
        second[c1:c2]
        .reshape(groups, rank_rows, chunk)
        .transpose(1, 0, 2)
        .reshape(rank_rows, grad_wkv.shape[1])
        .astype(f32)
    )
    small_own = exchange_tp(second[c2:].T)
    return (
        output,
        grad_input,
        small_own[:, s0],
        out_wq,
        small_own[:, :latent_count],
        small_own[:gain_rows, s0 + 2],
        out_wkv,
        out_wo,
        small_own[:, s0 + 1],
        small_own[:, latent_count:s0],
        first[:shared_width].T,
        first[shared_width : 2 * shared_width].T,
        first[2 * shared_width :].T,
        grad_expert_gate,
        grad_expert_up,
        grad_expert_down,
    )


def solution(mesh):
    in_specs = (
        P(("wide", "tp"), None),
        P(("wide", "tp"), None),
        P(("wide", "tp"), None),
        P(),
        P(None, "tp"),
        P(),
        P(),
        P(None, "tp"),
        P(None, "tp"),
        P(),
        P(),
        P(None, "tp"),
        P(None, "tp"),
        P(None, "tp"),
        P("wide", None, "tp"),
        P("wide", None, "tp"),
        P("wide", None, "tp"),
    )
    out_specs = (
        P(("wide", "tp"), None),
        P(("wide", "tp"), None),
        P(("wide", "tp")),
        P("wide", "tp"),
        P(("wide", "tp"), None),
        P(("wide", "tp")),
        P("wide", "tp"),
        P("wide", "tp"),
        P(("wide", "tp")),
        P(("wide", "tp"), None),
        P("wide", "tp"),
        P("wide", "tp"),
        P("wide", "tp"),
        P("wide", None, "tp"),
        P("wide", None, "tp"),
        P("wide", None, "tp"),
    )
    return jax.shard_map(
        on_device, mesh=mesh, in_specs=in_specs, out_specs=out_specs, check_vma=False
    )
```

```python
import jax
import jax.numpy as jnp
from jax import lax
from jax.experimental import pallas as pl
from jax.experimental.pallas import tpu as pltpu
from jax.sharding import PartitionSpec as P

NOPE = 128
ROPE = 64
VDIM = 128
RANK = 512


EPSILON = 1e-06
ROUTE_SCALE = 2.446
THETA = 50000.0
HIGHEST = lax.Precision.HIGHEST


def product(form, left, right):
    return jnp.einsum(form, left, right, preferred_element_type=jnp.float32)


def matmul_t(left, right):
    return lax.dot_general(
        left, right, (((1,), (1,)), ((), ())), preferred_element_type=jnp.float32
    )


def matmul_rows(left, right):
    return lax.dot_general(
        left, right, (((0,), (0,)), ((), ())), preferred_element_type=jnp.float32
    )


def rotary_tables(positions):
    half_width = ROPE // 2
    position = jnp.arange(positions, dtype=jnp.float32)[:, None]
    inverse = THETA ** (-jnp.arange(half_width, dtype=jnp.float32) / half_width)
    angle = position * inverse[None, :]
    return (jnp.cos(angle), jnp.sin(angle))


def rotate(vector, cosine, sine, turn):
    half_width = vector.shape[-1] // 2
    lower = vector[..., :half_width]
    upper = vector[..., half_width:]
    return jnp.concatenate(
        [lower * cosine - turn * upper * sine, upper * cosine + turn * lower * sine], axis=-1
    )


def rms_forward(vector, gain_vector):
    inv_scale = lax.rsqrt(jnp.mean(vector * vector, axis=-1, keepdims=True) + EPSILON)
    unit_rows = vector * inv_scale
    return (unit_rows, inv_scale, unit_rows * gain_vector)


def rms_backward(grad_normed, unit_rows, inv_scale, gain_vector):
    scaled = grad_normed * gain_vector
    grad_in = inv_scale * (
        scaled - unit_rows * jnp.mean(scaled * unit_rows, axis=-1, keepdims=True)
    )
    return (grad_in, jnp.sum(grad_normed * unit_rows, axis=0))


def score_block():
    return 512


def masked_scores(query_block, key_nope, key_rope):
    query_total = query_block.shape[0]
    key_total = key_nope.shape[0]
    scores = product("qhd,khd->hqk", query_block[..., :NOPE], key_nope)
    scores = scores + product("qhd,kd->hqk", query_block[..., NOPE:], key_rope)
    scores = scores * (NOPE + ROPE) ** (-0.5)
    query_pos = jnp.arange(query_total, dtype=jnp.int32)[:, None]
    key_pos = jnp.arange(key_total, dtype=jnp.int32)[None, :]
    return jnp.where((key_pos <= query_pos)[None], scores, -1e30)


def attention_forward(normed_b, w_query, w_latent, latent_gain, w_keyval, cosine, sine):
    row_total = normed_b.shape[0]
    head_count = w_keyval.shape[1] // (NOPE + VDIM)
    query_full = jnp.dot(normed_b, w_query, preferred_element_type=jnp.float32).reshape(
        row_total, head_count, NOPE + ROPE
    )
    query_b = jnp.concatenate(
        [
            query_full[..., :NOPE],
            rotate(query_full[..., NOPE:], cosine[:, None, :], sine[:, None, :], 1.0),
        ],
        axis=-1,
    ).astype(jnp.bfloat16)
    latent = jnp.dot(normed_b, w_latent, preferred_element_type=jnp.float32)
    key_rope = rotate(latent[:, RANK:], cosine, sine, 1.0).astype(jnp.bfloat16)
    latent_unit, latent_scale, latent_normed = rms_forward(latent[:, :RANK], latent_gain)
    latent_b = latent_normed.astype(jnp.bfloat16)
    keyval = (
        jnp.dot(latent_b, w_keyval, preferred_element_type=jnp.float32)
        .reshape(row_total, head_count, NOPE + VDIM)
        .astype(jnp.bfloat16)
    )
    key_nope = keyval[..., :NOPE]
    value_rows = keyval[..., NOPE:]
    scores = masked_scores(query_b, key_nope, key_rope)
    row_max = jnp.max(scores, axis=-1, keepdims=True)
    log_total = row_max + jnp.log(jnp.sum(jnp.exp(scores - row_max), axis=-1, keepdims=True))
    prob_b = jnp.exp(scores - log_total).astype(jnp.bfloat16)
    outputs = product("hqk,khd->qhd", prob_b, value_rows).astype(jnp.bfloat16)
    attn_b = outputs.reshape(row_total, head_count * VDIM)
    return (
        query_b,
        key_rope,
        latent_unit,
        latent_scale,
        latent_b,
        key_nope,
        value_rows,
        attn_b,
        log_total,
    )


def attention_backward(
    grad_attn_b, normed_b, saved, w_query, w_latent, latent_gain, w_keyval, cosine, sine
):
    (
        query_b,
        key_rope,
        latent_unit,
        latent_scale,
        latent_b,
        key_nope,
        value_rows,
        attn_b,
        log_sums,
    ) = saved
    row_total = normed_b.shape[0]
    head_count = key_nope.shape[1]
    grad_rows = grad_attn_b.reshape(row_total, head_count, VDIM)
    attn_rows = attn_b.reshape(row_total, head_count, VDIM)
    block_rows = score_block()
    scores = masked_scores(query_b, key_nope, key_rope)
    probs = jnp.exp(scores - log_sums)
    prob_b = probs.astype(jnp.bfloat16)
    grad_value = product("hqk,qhd->khd", prob_b, grad_rows)
    grad_probs = product("qhd,khd->hqk", grad_rows, value_rows)
    row_delta = jnp.sum(grad_rows.astype(jnp.float32) * attn_rows.astype(jnp.float32), axis=-1)
    grad_scores = (
        probs * (grad_probs - jnp.transpose(row_delta)[..., None]) * (NOPE + ROPE) ** (-0.5)
    ).astype(jnp.bfloat16)
    grad_query_nope = product("hqk,khd->qhd", grad_scores, key_nope)
    grad_query_rope = product("hqk,kd->qhd", grad_scores, key_rope)
    grad_queries = jnp.concatenate(
        [
            grad_query_nope,
            rotate(
                grad_query_rope, cosine[0:block_rows, None, :], sine[0:block_rows, None, :], -1.0
            ),
        ],
        axis=-1,
    )
    grad_key_nope = product("hqk,qhd->khd", grad_scores, query_b[..., :NOPE])
    grad_key_rope = product("hqk,qhd->kd", grad_scores, query_b[..., NOPE:])
    grad_query_b = grad_queries.reshape(row_total, head_count * (NOPE + ROPE)).astype(jnp.bfloat16)
    grad_keyval_b = (
        jnp.concatenate([grad_key_nope, grad_value], axis=-1)
        .reshape(row_total, head_count * (NOPE + VDIM))
        .astype(jnp.bfloat16)
    )
    grad_query_w = matmul_rows(grad_query_b, normed_b)
    grad_keyval_w = matmul_rows(latent_b, grad_keyval_b)
    grad_latent_normed = matmul_t(grad_keyval_b, w_keyval)
    grad_latent_core, grad_latent_gain = rms_backward(
        grad_latent_normed, latent_unit, latent_scale, latent_gain
    )
    grad_latent_rows = jnp.concatenate(
        [grad_latent_core, rotate(grad_key_rope, cosine, sine, -1.0)], axis=-1
    )
    normed_f = normed_b.astype(jnp.float32)
    grad_latent_w = jnp.dot(grad_latent_rows.T, normed_f, precision=HIGHEST)
    grad_normed = matmul_t(grad_query_b, w_query) + jnp.dot(
        grad_latent_rows, w_latent.astype(jnp.float32).T, precision=HIGHEST
    )
    return (grad_normed, grad_query_w, grad_latent_w, grad_latent_gain, grad_keyval_w)


def shared_forward(normed_b, gate_w, up_w):
    pre_gate = jnp.dot(normed_b, gate_w, preferred_element_type=jnp.float32)
    pre_up = jnp.dot(normed_b, up_w, preferred_element_type=jnp.float32)
    sigma_gate = jax.nn.sigmoid(pre_gate)
    activated = pre_gate * sigma_gate
    return (pre_gate, pre_up, sigma_gate, activated, (activated * pre_up).astype(jnp.bfloat16))


LANES = 128
VMEM_LIMIT = 64000000


def gather_tp(x):
    count = lax.axis_size("tp")
    at = lax.axis_index("tp")
    rows = x.shape[0]
    whole = jnp.zeros((count * rows, x.shape[1]), x.dtype)
    whole = lax.dynamic_update_slice_in_dim(whole, x, at * rows, 0)
    for step in range(1, count):
        came = lax.ppermute(x, "tp", [(i, (i + step) % count) for i in range(count)])
        whole = lax.dynamic_update_slice_in_dim(
            whole, came, ((at + count - step) % count) * rows, 0
        )
    return whole


def exchange_tp(x):
    count = lax.axis_size("tp")
    at = lax.axis_index("tp")
    rows = x.shape[0] // count
    total = lax.dynamic_slice_in_dim(x, at * rows, rows, 0).astype(jnp.float32)
    for step in range(1, count):
        part = lax.dynamic_slice_in_dim(x, ((at + step) % count) * rows, rows, 0)
        came = lax.ppermute(part, "tp", [(i, (i + step) % count) for i in range(count)])
        total = total + came.astype(jnp.float32)
    return total


def gather_wide(x):
    return lax.all_gather(x, "wide", axis=0, tiled=True)


def join_rows(parts):
    total = sum(part.shape[0] for part in parts)
    at = 0
    whole = None
    for part in parts:
        padded = jnp.pad(part, ((at, total - at - part.shape[0]), (0, 0)))
        whole = padded if whole is None else whole + padded
        at += part.shape[0]
    return whole


def scatter_wide_rows(x):
    return lax.psum_scatter(x, "wide", scatter_dimension=0, tiled=True)


def scatter_wide(x):
    return lax.psum_scatter(x, "wide", scatter_dimension=1, tiled=True)


def expert_front_kernel(
    blocks, slots, first_ref, x_ref, c_ref, router_ref, wg_ref, wu_ref, wd_ref,
    g_ref, xs_ref, cs_ref, hidden_ref, pg_ref, pu_ref, pick_ref, back_ref, gate_ref, sums_ref,
):
    f32, bf16 = jnp.float32, jnp.bfloat16
    width = x_ref.shape[1]
    own = x_ref.shape[0] // blocks
    experts = wg_ref.shape[0]
    slot_total = experts * slots
    first = first_ref[0, 0]
    sub = lax.broadcasted_iota(jnp.int32, (LANES, own), 0)
    above = (
        lax.broadcasted_iota(jnp.int32, (own, own), 0)
        < lax.broadcasted_iota(jnp.int32, (own, own), 1)
    ).astype(bf16)
    slot_ids = lax.broadcasted_iota(jnp.int32, (slots, own), 0).astype(f32)
    for b in range(blocks):
        rows = pl.ds(b * own, own)
        x_b = x_ref[rows, :]
        mask = c_ref[rows, width:].astype(f32)
        logits = jnp.dot(x_b, router_ref[...], preferred_element_type=f32)
        chosen = jax.nn.sigmoid(logits) * mask
        gate = ROUTE_SCALE * chosen / jnp.sum(chosen, axis=1, keepdims=True)
        gate_t = gate.T
        mask_t = mask.T
        place_t = jnp.dot(mask_t.astype(bf16), above, preferred_element_type=f32)
        picks = []
        for e in range(experts):
            here = sub == first + e
            mask_row = jnp.sum(jnp.where(here, mask_t, 0.0), axis=0, keepdims=True)
            place_row = jnp.sum(jnp.where(here, place_t, 0.0), axis=0, keepdims=True)
            gate_row = jnp.sum(jnp.where(here, gate_t, 0.0), axis=0, keepdims=True)
            pick = jnp.where(
                (slot_ids == place_row) & (mask_row > 0.0), jnp.ones_like(slot_ids), 0.0
            )
            picks.append(pick)
            gate_ref[e, pl.ds(b * slots, slots), :] = jnp.broadcast_to(
                jnp.sum(pick * gate_row, axis=1, keepdims=True), (slots, LANES)
            )
        pick_all = jnp.concatenate(picks, axis=0)
        pick_b = pick_all.astype(bf16)
        pick_ref[pl.ds(b * slot_total, slot_total), :] = pick_b
        x_s = jnp.dot(pick_b, x_b, preferred_element_type=f32).astype(bf16)
        c_s = jnp.dot(pick_b, c_ref[rows, :width], preferred_element_type=f32).astype(bf16)
        for e in range(experts):
            xs_ref[e, pl.ds(b * slots, slots), :] = x_s[e * slots : (e + 1) * slots]
            cs_ref[e, pl.ds(b * slots, slots), :] = c_s[e * slots : (e + 1) * slots]
    for e in range(experts):
        x_e = xs_ref[e]
        gate = gate_ref[e][:, :1]
        pre_gate = matmul_t(x_e, wg_ref[e])
        pre_up = matmul_t(x_e, wu_ref[e])
        grad_hidden = matmul_t(cs_ref[e], wd_ref[e])
        sigma = jax.nn.sigmoid(pre_gate)
        active = pre_gate * sigma
        hidden = active * pre_up
        sums_ref[e] = jnp.broadcast_to(
            jnp.sum(hidden * grad_hidden, axis=1, keepdims=True), sums_ref.shape[1:]
        )
        hidden_ref[e] = (hidden * gate).astype(bf16)
        weighted = grad_hidden * gate
        grad_pg = (weighted * pre_up * sigma * (1.0 + pre_gate * (1.0 - sigma))).astype(bf16)
        grad_pu = (weighted * active).astype(bf16)
        pg_ref[e] = grad_pg
        pu_ref[e] = grad_pu
        grad_in = (
            jnp.dot(grad_pg, wg_ref[e], preferred_element_type=f32)
            + jnp.dot(grad_pu, wu_ref[e], preferred_element_type=f32)
        ).astype(bf16)
        for b in range(blocks):
            back_ref[b, pl.ds(e * slots, slots), :] = grad_in[b * slots : (b + 1) * slots]
    for b in range(blocks):
        pick = pick_ref[pl.ds(b * slot_total, slot_total), :].astype(f32)
        sums_t = jnp.zeros((LANES, own), f32)
        for e in range(experts):
            row = jnp.sum(
                pick[e * slots : (e + 1) * slots] * sums_ref[e, pl.ds(b * slots, slots), :][:, :1],
                axis=0,
                keepdims=True,
            )
            sums_t = sums_t + jnp.where(sub == first + e, row, 0.0)
        rows = pl.ds(b * own, own)
        g_ref[rows, width:] = sums_t.T.astype(bf16)
        g_ref[rows, :width] = jnp.dot(
            pick.T.astype(bf16), back_ref[b], preferred_element_type=f32
        ).astype(bf16)


def expert_front(first, rows_x, rows_c, router, w_gate, w_up, w_down, blocks, slots, own):
    bf16 = jnp.bfloat16
    total, width = rows_x.shape
    experts, hidden, _ = w_gate.shape
    step_rows = blocks * own
    steps = total // step_rows
    step_slots = blocks * slots
    all_slots = steps * step_slots

    def whole(shape):
        return pl.BlockSpec(shape, lambda i: (0,) * len(shape), pipeline_mode=pl.Buffered(1))

    def per_expert(last):
        return pl.BlockSpec((experts, step_slots, last), lambda i: (0, i, 0))

    flops = 2 * all_slots * experts * width * (5 * hidden + 2 * own) + 2 * total * width * LANES
    return pl.pallas_call(
        lambda *refs: expert_front_kernel(blocks, slots, *refs),
        grid=(steps,),
        in_specs=[
            pl.BlockSpec(memory_space=pltpu.SMEM),
            pl.BlockSpec((step_rows, width), lambda i: (i, 0)),
            pl.BlockSpec((step_rows, width + LANES), lambda i: (i, 0)),
            whole((width, LANES)),
            whole(w_gate.shape),
            whole(w_up.shape),
            whole(w_down.shape),
        ],
        out_specs=[
            pl.BlockSpec((step_rows, width + LANES), lambda i: (i, 0)),
            per_expert(width),
            per_expert(width),
            per_expert(hidden),
            per_expert(hidden),
            per_expert(hidden),
            pl.BlockSpec((blocks * experts * slots, own), lambda i: (i, 0)),
        ],
        out_shape=[
            jax.ShapeDtypeStruct((total, width + LANES), bf16),
            jax.ShapeDtypeStruct((experts, all_slots, width), bf16),
            jax.ShapeDtypeStruct((experts, all_slots, width), bf16),
            jax.ShapeDtypeStruct((experts, all_slots, hidden), bf16),
            jax.ShapeDtypeStruct((experts, all_slots, hidden), bf16),
            jax.ShapeDtypeStruct((experts, all_slots, hidden), bf16),
            jax.ShapeDtypeStruct((total // own * experts * slots, own), bf16),
        ],
        scratch_shapes=[
            pltpu.VMEM((blocks, experts * slots, width), bf16),
            pltpu.VMEM((experts, step_slots, LANES), jnp.float32),
            pltpu.VMEM((experts, step_slots, LANES), jnp.float32),
        ],
        compiler_params=pltpu.CompilerParams(vmem_limit_bytes=VMEM_LIMIT),
        cost_estimate=pl.CostEstimate(
            flops=flops,
            bytes_accessed=2 * width * (3 * total + 2 * experts * all_slots),
            transcendentals=0,
        ),
        name="expert_front",
    )(first, rows_x, rows_c, router, w_gate, w_up, w_down)


def expert_out_kernel(blocks, slots, hidden_ref, pick_ref, wd_ref, y_ref, rows_ref):
    f32, bf16 = jnp.float32, jnp.bfloat16
    experts = wd_ref.shape[0]
    own = y_ref.shape[0] // blocks
    for e in range(experts):
        out = jnp.dot(hidden_ref[e], wd_ref[e], preferred_element_type=f32).astype(bf16)
        for b in range(blocks):
            rows_ref[b, pl.ds(e * slots, slots), :] = out[b * slots : (b + 1) * slots]
    for b in range(blocks):
        pick = pick_ref[pl.ds(b * experts * slots, experts * slots), :].astype(f32)
        y_ref[pl.ds(b * own, own), :] = jnp.dot(
            pick.T.astype(bf16), rows_ref[b], preferred_element_type=f32
        ).astype(bf16)


def expert_out(hidden, picks, w_down, blocks, slots, own):
    bf16 = jnp.bfloat16
    experts, units, width = w_down.shape
    total = picks.shape[0] // (experts * slots) * own
    step_rows = blocks * own
    step_slots = blocks * slots
    steps = total // step_rows
    return pl.pallas_call(
        lambda *refs: expert_out_kernel(blocks, slots, *refs),
        grid=(steps,),
        in_specs=[
            pl.BlockSpec((experts, step_slots, units), lambda i: (0, i, 0)),
            pl.BlockSpec((blocks * experts * slots, own), lambda i: (i, 0)),
            pl.BlockSpec(
                w_down.shape, lambda i: (0, 0, 0), pipeline_mode=pl.Buffered(1)
            ),
        ],
        out_specs=pl.BlockSpec((step_rows, width), lambda i: (i, 0)),
        out_shape=jax.ShapeDtypeStruct((total, width), bf16),
        scratch_shapes=[pltpu.VMEM((blocks, experts * slots, width), bf16)],
        compiler_params=pltpu.CompilerParams(vmem_limit_bytes=VMEM_LIMIT),
        cost_estimate=pl.CostEstimate(
            flops=2 * steps * step_slots * experts * width * (units + own),
            bytes_accessed=2 * total * width,
            transcendentals=0,
        ),
        name="expert_out",
    )(hidden, picks, w_down)


def on_device(
    inputs,
    cotangent,
    expert_choice,
    norm1_gain,
    w_query,
    w_latent,
    latent_gain,
    w_keyval,
    w_out,
    norm2_gain,
    w_router,
    w_shared_gate,
    w_shared_up,
    w_shared_down,
    w_expert_gate,
    w_expert_up,
    w_expert_down,
):
    bf16 = jnp.bfloat16
    f32 = jnp.float32
    tp_count = lax.axis_size("tp")
    wide_count = lax.axis_size("wide")
    wide_at = lax.axis_index("wide")
    own_count, width = inputs.shape
    top_count = expert_choice.shape[1]
    expert_total = w_router.shape[1]
    local_experts = w_expert_gate.shape[0]
    capacity = 8 * (own_count * top_count // (8 * expert_total) + 1)
    slots = -(-capacity // 16) * 16
    seq_rows = own_count * tp_count
    all_rows = seq_rows * wide_count
    blocks = wide_count * tp_count

    chosen_own = jnp.any(
        expert_choice[:, :, None] == jnp.arange(expert_total, dtype=jnp.int32), axis=1
    )
    mask_own = chosen_own.astype(f32)
    input_all = gather_tp(inputs)
    early = jnp.concatenate(
        [cotangent, jnp.pad(mask_own, ((0, 0), (0, LANES - expert_total))).astype(bf16)], axis=1
    )
    input_all, early = lax.optimization_barrier((input_all, early))
    early_seq = gather_tp(early)

    cosine, sine = rotary_tables(seq_rows)
    unit1, _, normed1 = rms_forward(input_all.astype(f32), norm1_gain)
    normed1_b = normed1.astype(bf16)
    saved = attention_forward(normed1_b, w_query, w_latent, latent_gain, w_keyval, cosine, sine)
    attn_part = matmul_t(saved[7], w_out).astype(bf16)
    attn_part, early_seq = lax.optimization_barrier((attn_part, early_seq))
    early_all = gather_wide(early_seq)
    cot_seq = early_seq[:, :width]
    attn_own = exchange_tp(attn_part)
    input_own = inputs.astype(f32)
    hidden_own = input_own + attn_own
    unit2, scale2, normed2 = rms_forward(hidden_own, norm2_gain)
    normed2_own = normed2.astype(bf16)
    normed2_seq = gather_tp(normed2_own)
    gather_from, early_all = lax.optimization_barrier((normed2_seq, early_all))
    normed2_all = gather_wide(gather_from)

    pre_gate, pre_up, sigma_gate, activated, shared_b = shared_forward(
        normed2_seq, w_shared_gate, w_shared_up
    )
    shared_part = matmul_t(shared_b, w_shared_down)
    grad_shared_hidden = jnp.dot(cot_seq, w_shared_down, preferred_element_type=f32)
    grad_pre_gate_b = (
        grad_shared_hidden * pre_up * sigma_gate * (1.0 + pre_gate * (1.0 - sigma_gate))
    ).astype(bf16)
    grad_pre_up_b = (grad_shared_hidden * activated).astype(bf16)
    grad_shared = jnp.concatenate(
        [
            matmul_rows(grad_pre_gate_b, normed2_seq).astype(bf16),
            matmul_rows(grad_pre_up_b, normed2_seq).astype(bf16),
            matmul_rows(shared_b, cot_seq).astype(bf16),
        ],
        axis=0,
    )
    shared_back = matmul_t(grad_pre_gate_b, w_shared_gate) + matmul_t(grad_pre_up_b, w_shared_up)
    first_expert = (wide_at * local_experts).astype(jnp.int32).reshape(1, 1)
    first_expert, shared_part, shared_back, grad_shared = lax.optimization_barrier(
        (first_expert, shared_part, shared_back, grad_shared)
    )
    first = scatter_wide(grad_shared)

    grad_in_all, x_slots, c_slots, hidden_slots, pg_slots, pu_slots, picks = expert_front(
        first_expert,
        normed2_all,
        early_all,
        jnp.pad(w_router, ((0, 0), (0, LANES - expert_total))),
        jnp.swapaxes(w_expert_gate, 1, 2),
        jnp.swapaxes(w_expert_up, 1, 2),
        jnp.swapaxes(w_expert_down, 1, 2),
        tp_count,
        slots,
        own_count,
    )
    grad_in_all, first = lax.optimization_barrier((grad_in_all, first))
    first = first.astype(f32)
    grad_in_seq = scatter_wide_rows(grad_in_all)
    out_all = expert_out(
        hidden_slots, picks, jnp.swapaxes(w_expert_down, 1, 2), tp_count, slots, own_count
    )
    out_seq = scatter_wide_rows(out_all)
    grad_expert_gate = product("emd,emf->edf", x_slots, pg_slots)
    grad_expert_up = product("emd,emf->edf", x_slots, pu_slots)
    grad_expert_down = product("emd,emf->edf", c_slots, hidden_slots)
    grad_in_seq, grad_expert_gate, grad_expert_up, grad_expert_down = lax.optimization_barrier(
        (grad_in_seq, grad_expert_gate, grad_expert_up, grad_expert_down)
    )

    back = (
        grad_in_seq.astype(f32) + jnp.pad(shared_back, ((0, 0), (0, LANES)))
    ).astype(bf16)
    back_own = exchange_tp(back)
    grad_gate = back_own[:, width : width + expert_total]
    logits = jnp.dot(normed2_own, w_router, preferred_element_type=f32)
    selected = jax.nn.sigmoid(logits)
    sel_total = jnp.sum(selected * mask_own, axis=1, keepdims=True)
    weighted = jnp.sum(grad_gate * selected * mask_own, axis=1, keepdims=True)
    grad_selected = ROUTE_SCALE * (grad_gate / sel_total - weighted / (sel_total * sel_total))
    grad_logits = grad_selected * selected * (1.0 - selected) * mask_own
    grad_router = jnp.dot(grad_logits.T, normed2_own.astype(f32), precision=HIGHEST)
    grad_normed2 = back_own[:, :width] + jnp.dot(
        grad_logits, w_router.astype(f32).T, precision=HIGHEST
    )
    grad_h2, grad_g2 = rms_backward(grad_normed2, unit2, scale2, norm2_gain)
    grad_hidden_own = cotangent.astype(f32) + grad_h2
    grad_hidden_b = gather_tp(grad_hidden_own.astype(bf16))

    grad_wo = matmul_rows(saved[7], grad_hidden_b).astype(bf16)
    grad_attn_b = jnp.dot(grad_hidden_b, w_out, preferred_element_type=f32).astype(bf16)
    grad_normed1, grad_wq, grad_wlat, grad_lgain, grad_wkv = attention_backward(
        grad_attn_b, normed1_b, saved, w_query, w_latent, latent_gain, w_keyval, cosine, sine
    )
    grad_g1 = jnp.sum(grad_normed1 * unit1, axis=0)
    grad_normed1_own = exchange_tp(grad_normed1.astype(bf16))
    output = hidden_own + exchange_tp((out_seq.astype(f32) + shared_part).astype(bf16))
    chunk = width // wide_count
    shared_width = shared_b.shape[1]
    rank = latent_gain.shape[0]
    gain_rows = rank // blocks
    lgain_row = jnp.pad(
        grad_lgain.reshape(blocks, gain_rows), ((0, 0), (0, width // blocks - gain_rows))
    ).reshape(1, width)
    latent_count = grad_wlat.shape[0]
    s0 = latent_count + expert_total
    gains = jnp.concatenate(
        [grad_g1[None], grad_g2[None], lgain_row, jnp.zeros((13, width), f32)], axis=0
    )
    rank_rows = rank // wide_count
    groups = grad_wkv.shape[1] // chunk
    folded = (
        grad_wkv.astype(bf16)
        .reshape(wide_count, rank_rows, groups, chunk)
        .transpose(2, 1, 0, 3)
        .reshape(groups * rank_rows, width)
    )
    second = scatter_wide(
        join_rows(
            [
                grad_wo,
                grad_wq.astype(bf16),
                folded,
                grad_wlat.astype(bf16),
                grad_router.astype(bf16),
                gains.astype(bf16),
            ]
        )
    )
    c0 = grad_wo.shape[0]
    c1 = c0 + grad_wq.shape[0]
    c2 = c1 + groups * rank_rows
    out_wo = second[:c0].astype(f32).T
    out_wq = second[c0:c1].astype(f32).T
    out_wkv = (
        second[c1:c2]
        .reshape(groups, rank_rows, chunk)
        .transpose(1, 0, 2)
        .reshape(rank_rows, grad_wkv.shape[1])
        .astype(f32)
    )
    small, grad_normed1_own = lax.optimization_barrier((second[c2:], grad_normed1_own))
    small_own = lax.psum_scatter(
        small.T, "tp", scatter_dimension=0, tiled=True
    ).astype(f32)
    scaled = grad_normed1_own * norm1_gain
    unit1_own, scale1_own, _ = rms_forward(input_own, norm1_gain)
    grad_input = grad_hidden_own + scale1_own * (
        scaled - unit1_own * jnp.mean(scaled * unit1_own, axis=-1, keepdims=True)
    )
    return (
        output,
        grad_input,
        small_own[:, s0],
        out_wq,
        small_own[:, :latent_count],
        small_own[:gain_rows, s0 + 2],
        out_wkv,
        out_wo,
        small_own[:, s0 + 1],
        small_own[:, latent_count:s0],
        first[:shared_width].T,
        first[shared_width : 2 * shared_width].T,
        first[2 * shared_width :].T,
        grad_expert_gate,
        grad_expert_up,
        grad_expert_down,
    )


def solution(mesh):
    in_specs = (
        P(("wide", "tp"), None),
        P(("wide", "tp"), None),
        P(("wide", "tp"), None),
        P(),
        P(None, "tp"),
        P(),
        P(),
        P(None, "tp"),
        P(None, "tp"),
        P(),
        P(),
        P(None, "tp"),
        P(None, "tp"),
        P(None, "tp"),
        P("wide", None, "tp"),
        P("wide", None, "tp"),
        P("wide", None, "tp"),
    )
    out_specs = (
        P(("wide", "tp"), None),
        P(("wide", "tp"), None),
        P(("wide", "tp")),
        P("wide", "tp"),
        P(("wide", "tp"), None),
        P(("wide", "tp")),
        P("wide", "tp"),
        P("wide", "tp"),
        P(("wide", "tp")),
        P(("wide", "tp"), None),
        P("wide", "tp"),
        P("wide", "tp"),
        P("wide", "tp"),
        P("wide", None, "tp"),
        P("wide", None, "tp"),
        P("wide", None, "tp"),
    )
    return jax.shard_map(
        on_device, mesh=mesh, in_specs=in_specs, out_specs=out_specs, check_vma=False
    )
```
